32 devices in a mesh: ens: 2 (over y), box: 4 (over z), slab: 4 (over x, core).
Axes of the slice: x: 2, y: 2, z: 4, core: 2. Of those that a mesh axis runs over, the one named last changes fastest.
Arguments:
- pressure_now: float32 [4, 64, 64, 256], P('ens', 'box', 'slab'), parts along dimension 0, may hold values from -6 to 6
- pressure_prev: float32 [4, 64, 64, 256], P('ens', 'box', 'slab'), parts along dimension 0, may hold values from -6 to 6
- courant_sq: float32 [64, 64, 256], P('box', 'slab'), may hold values from 0.04 to 0.28
- member_profiles: float32 [8, 64], replicated, may hold values from -0.15 to 0.15
- member_ids: int32 [4], P('ens'), parts along dimension 0, may hold values from 0 to 7, as said below
- stored_slabs: float32 [8, 16, 6144], P('slab'), may hold values from -6 to 6
- slab_home: int32 [2], P('ens'), parts along dimension 0, may hold values from 0 to 7
- interp_weights: float32 [2, 16], replicated, may hold values from -1.5 to 1.5
- surface_cells: int32 [6, 1024], replicated, may hold values from 0 to 1048575, as said below
Outputs:
- pressure_next: float32 [4, 64, 64, 256], P('ens', 'box', 'slab'), parts along dimension 0
- pressure_last: float32 [4, 64, 64, 256], P('ens', 'box', 'slab'), parts along dimension 0
The draws below stay inside these ranges and needn't reach their ends.
There are 2 independent parts, one for each index of `ens`. The reference program is written for one: setup_inputs(seed, part) draws one part's arguments, and reference() takes and returns one part's arrays. A program takes and returns all parts, laid end to end along the dimension named above; an argument that names none is the same for every part. Nothing has to cross between parts.
Inputs may be any that keep to these rules, and one draw needn't show every extreme that they name: `surface_cells`: row f lists 1024 cells, flat index (x 64 + z) * 256 + y, on one face of the box surface 0 cells inside the grid: x low, x high, z low, z high, y low, y high in this order; the other two coordinates lie on the surface; on every face other than the two depth faces, every depth of the surface occurs; cells may repeat. `slab_home`: block k is stored on the slab device k // 2, in its slot k % 2. `member_ids`: the members' profiles are all different.
All inputs are finite; a program needn't handle non-finite values.
Results may differ from the reference program's by a relative error of at most 0.000098.
Values sent between devices are 32-bit elements; how exact they have to be, the bound alone decides.
A program may use at most 64 MiB of HBM per device.

```python
import math
import jax
import jax.numpy as jnp
from jax import lax

MEMBERS = 2
STEPS = 2
SLAB_LEN = 16
BANK = 8
HUYGENS_GAP = 0
NY = 256
PTS_FACE = 1024
NX = 64
NZ = 64
BLOCKS = 8
POINTS = 6144


def draw_member_ids(key, part):
    order = jax.random.permutation(jax.random.fold_in(key, 29), jnp.arange(BANK, dtype=jnp.int32))
    return order[:MEMBERS].astype(jnp.int32)


def draw_surface_cells(key, part):
    subkeys = jax.random.split(jax.random.fold_in(key, 17), 4)
    face_index = jnp.arange(6, dtype=jnp.int32)[:, None]
    point_index = jnp.arange(PTS_FACE, dtype=jnp.int32)[None, :]
    along_x = jax.random.randint(subkeys[0], (6, PTS_FACE), HUYGENS_GAP, NX - HUYGENS_GAP)
    along_z = jax.random.randint(subkeys[1], (6, PTS_FACE), HUYGENS_GAP, NZ - HUYGENS_GAP)
    along_y = jax.random.randint(subkeys[2], (6, PTS_FACE), HUYGENS_GAP, NY - HUYGENS_GAP)
    depth_span = NZ - 2 * HUYGENS_GAP
    offset = jax.random.randint(subkeys[3], (6, 1), 0, depth_span)
    covering = HUYGENS_GAP + (point_index + offset) % depth_span
    along_z = jnp.where(point_index < depth_span, covering, along_z)
    along_x = jnp.where(face_index == 0, HUYGENS_GAP, jnp.where(face_index == 1, NX - 1 - HUYGENS_GAP, along_x))
    along_z = jnp.where(face_index == 2, HUYGENS_GAP, jnp.where(face_index == 3, NZ - 1 - HUYGENS_GAP, along_z))
    along_y = jnp.where(face_index == 4, HUYGENS_GAP, jnp.where(face_index == 5, NY - 1 - HUYGENS_GAP, along_y))
    return ((along_x * NZ + along_z) * NY + along_y).astype(jnp.int32)


def levels(own_key, extent, cuts, smallest, high):
    gain, own = 1.0, jax.random.fold_in(own_key, 6)
    for position, parts in cuts:
        heights = jnp.exp(jax.random.uniform(jax.random.fold_in(own, position), (parts,), jnp.float32, smallest / len(cuts), high / len(cuts)))
        gain = gain * jnp.repeat(heights, extent[position] // parts).reshape([-1 if axis == position else 1 for axis in range(len(extent))])
    return gain


def gaussian(rng, shape, width, reach, cuts=(), kind=jnp.bfloat16):
    values = jax.random.normal(rng, shape, jnp.float32) * width
    if len(cuts) > 0:
        values = levels(rng, shape, cuts, -0.22, 0.18) * values
    return jnp.clip(values, min=-reach, max=reach).astype(kind)


def setup_inputs(seed: int = 0, part: int = 0) -> dict:
    arg_keys = jax.random.split(jax.random.key(seed), 10)
    part_splits = jax.random.split(jax.random.fold_in(arg_keys[9], part), 10)
    pressure_now = gaussian(part_splits[0], (MEMBERS, NX, NZ, NY), 1.0, 6.0, ((1, 4), (2, 4)), jnp.float32)
    pressure_prev = gaussian(part_splits[1], (MEMBERS, NX, NZ, NY), 1.0, 6.0, ((1, 4), (2, 4)), jnp.float32)
    courant_sq = jnp.clip(jnp.exp(math.log(0.28) - 1.9459102 * jax.random.uniform(arg_keys[2], (NX, NZ, NY), jnp.float32) ** levels(arg_keys[2], (NX, NZ, NY), ((0, 4), (1, 4)), -0.2, 0.2)), 0.04, 0.28)
    member_profiles = jnp.clip(jax.random.uniform(arg_keys[3], (BANK, NZ), jnp.float32, -0.15, 0.15), -0.15, 0.15)
    member_ids = draw_member_ids(jax.random.fold_in(jax.random.fold_in(arg_keys[9], part), 71), part)
    stored_slabs = gaussian(arg_keys[5], (BLOCKS, SLAB_LEN, POINTS), 1.0, 6.0, ((0, 4),), jnp.float32)
    slab_home = jax.random.randint(part_splits[6], (1,), 0, BLOCKS).astype(jnp.int32)
    interp_weights = gaussian(arg_keys[7], (STEPS, SLAB_LEN), 0.3, 1.5, (), jnp.float32)
    surface_cells = draw_surface_cells(jax.random.fold_in(arg_keys[9], 71), part)
    return {"pressure_now": pressure_now, "pressure_prev": pressure_prev, "courant_sq": courant_sq, "member_profiles": member_profiles, "member_ids": member_ids, "stored_slabs": stored_slabs, "slab_home": slab_home, "interp_weights": interp_weights, "surface_cells": surface_cells}


def laplace(ext):
    inner = ext[:, 1:-1, 1:-1, :]
    beside = ext[:, 2:, 1:-1, :] + ext[:, :-2, 1:-1, :]
    beside = beside + ext[:, 1:-1, 2:, :] + ext[:, 1:-1, :-2, :]
    padded = jnp.pad(inner, ((0, 0), (0, 0), (0, 0), (1, 1)))
    beside = beside + padded[:, :, :, 2:] + padded[:, :, :, :-2]
    return beside - 6.0 * inner


def reference(pressure_now, pressure_prev, courant_sq, member_profiles, member_ids, stored_slabs, slab_home, interp_weights, surface_cells):
    profile = member_profiles[member_ids]
    coef = courant_sq[None] * (1.0 + profile[:, None, :, None])
    block = lax.dynamic_index_in_dim(stored_slabs, slab_home[0], 0, keepdims=False)
    values = jnp.dot(interp_weights, block, precision=lax.Precision.HIGHEST)
    cells = surface_cells.reshape(-1)
    prev, now = pressure_prev, pressure_now
    for step in range(STEPS):
        ext = jnp.pad(now, ((0, 0), (1, 1), (1, 1), (0, 0)))
        nxt = 2.0 * now - prev + coef * laplace(ext)
        source = jnp.zeros((NX * NZ * NY,), jnp.float32).at[cells].add(values[step])
        nxt = nxt + source.reshape(NX, NZ, NY)[None]
        prev, now = now, nxt
    return now, prev
```

```python
import functools

import jax
import jax.numpy as jnp
from jax import lax
from jax.experimental import pallas as pl
from jax.experimental.pallas import tpu as pltpu
from jax.sharding import PartitionSpec as P

F32, BF16, I32 = jnp.float32, jnp.bfloat16, jnp.int32
MESH = pl.DeviceIdType.MESH
MARGIN, WIDE = 8, 128


def iota(shape, dim):
    return lax.broadcasted_iota(I32, shape, dim)


def quotient(values, divisor):
    if divisor & (divisor - 1) == 0:
        return lax.shift_right_logical(values, divisor.bit_length() - 1)
    return lax.div(values, jnp.full_like(values, divisor))


def split2(v):
    high = v.astype(BF16).astype(F32)
    return high, v - high


def place(row_hot, values, right):
    rows = row_hot.shape[0]
    parts = []
    for v in values:
        for term in split2(v):
            wide = jnp.broadcast_to(term, (16, v.shape[1])).astype(BF16)
            parts += [row_hot[r : r + 16, :] * wide for r in range(0, rows, 16)]
    left = jnp.concatenate(parts, axis=0)
    sums = lax.dot_general(left, right[...], (((1,), (1,)), ((), ())), preferred_element_type=F32)
    return [sums[2 * t * rows : (2 * t + 1) * rows] + sums[(2 * t + 1) * rows : (2 * t + 2) * rows]
            for t in range(len(values))]


def along_y(c, y_at):
    ny = c.shape[1]
    return (jnp.where(y_at == 0, 0.0, pltpu.roll(c, 1, 1))
            + jnp.where(y_at == ny - 1, 0.0, pltpu.roll(c, ny - 1, 1)))


def kernel(dims, home, ids_h, prof_h, weights_h, cells_h, now_h, prev_h, cour_h, slabs_h,
           one, now, coef, xout, zout, src,
           ids, prof, weights, cells, prev, cour, slab_y, slab_z, slab_x,
           psend, zsend, zpsend, csend, xghost, xcour, xpart, zghost, zpart, corner,
           row_x, row_z, row_low, row_high, hot_x, hot_z, hot_low, hot_high,
           ysend, xvsend, zvsend, yrecv, xvrecv, zvrecv,
           load_sem, hs_sem, hr_sem, cs_sem, cr_sem, vs_sem, vr_sem, diag_sem):
    members, wx, wz, ny, slots, length, pts, n_box, n_slab = dims
    steps = 2
    block = wx * wz
    box, slab = lax.axis_index("box"), lax.axis_index("slab")
    face_x = jnp.where(box == 0, 0, 1)
    box_edge = (box == 0) | (box == n_box - 1)
    slab_edge = (slab == 0) | (slab == n_slab - 1)
    pairs = (
        (slabs_h.at[:, pl.ds(4 * pts, 2 * pts)], slab_y), (weights_h, weights),
        (slabs_h.at[:, pl.ds(2 * pts, 2 * pts)], slab_z),
        (slabs_h.at[:, pl.ds(pl.multiple_of(face_x * pts, 128), pts)], slab_x),
        (now_h, now), (cour_h, cour), (prof_h, prof), (ids_h, ids), (prev_h, prev), (cells_h, cells))
    loads = [pltpu.make_async_copy(src_, dst, load_sem.at[i]) for i, (src_, dst) in enumerate(pairs)]
    for c in loads[:4]:
        c.start()

    barrier = pltpu.get_barrier_semaphore()

    def greet(target):
        pl.semaphore_signal(barrier, inc=1, device_id=target, device_id_type=MESH)

    sends_box = (box < n_box - 1, box > 0)
    sends_slab = (slab < n_slab - 1, slab > 0)
    hears_box = (box > 0, box < n_box - 1)
    hears_slab = (slab > 0, slab < n_slab - 1)
    shift = (1, -1)

    for d in range(1, n_slab):
        greet({"slab": lax.rem(slab + d, n_slab)})
    for a in range(2):
        @pl.when(sends_box[a])
        def _(a=a):
            greet({"box": box + shift[a]})
    for c in loads[4:]:
        c.start()

    for i in range(4):
        loads[i].wait()
    eye = iota((length, length), 0) == iota((length, length), 1)
    cols = []
    for t in range(steps):
        col = jnp.sum(jnp.where(eye, weights[t : t + 1, :], 0.0), axis=1, keepdims=True)
        cols.append([jnp.where(home[0] == slab * slots + s, col, 0.0) for s in range(slots)])

    def offered(ref, at, t):
        where = pl.ds(at, pts)
        total = cols[t][0] * ref[pl.ds(0, length), where]
        for s in range(1, slots):
            total = total + cols[t][s] * ref[pl.ds(s * length, length), where]
        return jnp.sum(total, axis=0, keepdims=True)

    both = range(steps)
    ysend[...] = jnp.concatenate([offered(slab_y, f * pts, t) for f in range(2) for t in both], axis=0)
    for f in range(2):
        zvsend[f] = jnp.concatenate([offered(slab_z, f * pts, t) for t in both], axis=0)
    xvsend[...] = jnp.concatenate([offered(slab_x, 0, t) for t in both], axis=0)

    loads[4].wait()
    loads[5].wait()
    edge_x, edge_z = (wx - 1, 0), (wz - 1, 0)
    for b in range(2):
        for x in range(wx):
            for m in range(members):
                zsend[b, m, x : x + 1, :] = now[pl.ds((m * wx + x) * wz + edge_z[b], 1), :]
            zsend[b, members, x : x + 1, :] = cour[pl.ds(x * wz + edge_z[b], 1), :]
        for a in range(2):
            for m in range(members):
                csend[a, b, m : m + 1, :] = now[pl.ds((m * wx + edge_x[a]) * wz + edge_z[b], 1), :]

    def give(d, kind):
        peer = lax.rem(slab + d, n_slab)
        ref, into = ((ysend, yrecv), (xvsend, xvrecv), (zvsend.at[0], zvrecv), (zvsend.at[1], zvrecv))[kind]
        k = min(kind, 2)
        return pltpu.make_async_remote_copy(
            ref, into.at[d - 1], vs_sem.at[d - 1, k], vr_sem.at[d - 1, k],
            device_id={"slab": peer}, device_id_type=MESH)

    def gives(d, kind):
        peer = lax.rem(slab + d, n_slab)
        return (None, box_edge, peer == 0, peer == n_slab - 1)[kind]

    def each_give(act):
        for d in range(1, n_slab):
            for kind in range(4):
                cond = gives(d, kind)
                if cond is None:
                    act(give(d, kind))
                else:
                    @pl.when(cond)
                    def _(d=d, kind=kind):
                        act(give(d, kind))

    given, parts = range(members + 1), range(members + 1, members + 2)

    def x_copies(a, which):
        peer = {"box": box + shift[a]}
        refs = [(now.at[pl.ds((m * wx + edge_x[a]) * wz, wz)], xghost.at[a, m]) for m in range(members)]
        refs += [(cour.at[pl.ds(edge_x[a] * wz, wz)], xcour.at[a]), (psend.at[a], xpart.at[a])]
        return [pltpu.make_async_remote_copy(*refs[i], hs_sem.at[a, i], hr_sem.at[a, i], device_id=peer, device_id_type=MESH)
                for i in which]

    def z_copy(b, i):
        source_, target = ((zsend.at[b], zghost.at[b]), (zpsend.at[b], zpart.at[b]))[i]
        return pltpu.make_async_remote_copy(source_, target, hs_sem.at[2 + b, i], hr_sem.at[2 + b, i],
                                            device_id={"slab": slab + shift[b]}, device_id_type=MESH)

    def corner_copy(a, b):
        return pltpu.make_async_remote_copy(
            csend.at[a, b], corner.at[a, b], cs_sem.at[a, b], cr_sem.at[a, b],
            device_id={"box": box + shift[a], "slab": slab + shift[b]}, device_id_type=MESH)

    box_peers = jnp.where(box > 0, 1, 0) + jnp.where(box < n_box - 1, 1, 0)
    pl.semaphore_wait(barrier, n_slab - 1 + box_peers)
    for a in range(2):
        @pl.when(sends_box[a])
        def _(a=a):
            pl.semaphore_signal(diag_sem.at[a], inc=1, device_id={"box": box + shift[a]}, device_id_type=MESH)
            for c in x_copies(a, given):
                c.start()
    each_give(lambda c: c.start())
    for b in range(2):
        @pl.when(sends_slab[b])
        def _(b=b):
            z_copy(b, 0).start()

    loads[6].wait()
    loads[7].wait()
    bank, total_z = prof.shape
    here = iota((wz, total_z), 1) == slab * wz + iota((wz, total_z), 0)
    beyond = [iota((1, total_z), 1) == slab * wz + at for at in (-1, wz)]
    gains, gains_beyond = [], []
    for m in range(members):
        mine = jnp.sum(jnp.where(iota((bank, total_z), 0) == ids[m], prof[...], 0.0), axis=0, keepdims=True)
        gains.append(1.0 + jnp.sum(jnp.where(here, mine, 0.0), axis=1, keepdims=True))
        gains_beyond.append([1.0 + jnp.sum(jnp.where(at, mine, 0.0), axis=1, keepdims=True) for at in beyond])

    loads[8].wait()
    z_at, y_at, x_at = iota((wz, ny), 0), iota((wz, ny), 1), iota((wx, ny), 0)
    for m in range(members):
        for x in (0, wx - 1, *range(1, wx - 1)):
            at = (m * wx + x) * wz
            rows = pl.ds(at, wz)
            c = now[rows, :]
            k = cour[pl.ds(x * wz, wz), :] * gains[m]
            coef[rows, :] = k
            lap = along_y(c, y_at) - 6.0 * c
            if x > 0:
                lap = lap + now[pl.ds(at - wz, wz), :]
            if x < wx - 1:
                lap = lap + now[pl.ds(at + wz, wz), :]
            lap = lap + jnp.where(z_at == 0, 0.0, pltpu.roll(c, 1, 0))
            lap = lap + jnp.where(z_at == wz - 1, 0.0, pltpu.roll(c, wz - 1, 0))
            nxt = (2.0 * c - prev[rows, :]) + k * lap
            if x == wx - 1:
                psend[0, m] = nxt
            elif x == 0:
                psend[1, m] = nxt
            else:
                one[rows, :] = nxt
            for b in range(2):
                zpsend[b, m, x : x + 1, :] = nxt[edge_z[b] : edge_z[b] + 1, :]
    for a in range(2):
        @pl.when(sends_box[a])
        def _(a=a):
            x_copies(a, parts)[0].start()
    for b in range(2):
        @pl.when(sends_slab[b])
        def _(b=b):
            z_copy(b, 1).start()

    for a in range(2):
        @pl.when(hears_box[1 - a])
        def _(a=a):
            pl.semaphore_wait(diag_sem.at[1 - a], 1)
            for b in range(2):
                @pl.when(sends_slab[b])
                def _(b=b):
                    corner_copy(a, b).start()

    loads[9].wait()

    def where_is(face):
        cell = cells[pl.ds(face, 1), :]
        cx = quotient(cell, total_z * ny)
        rest = cell - cx * (total_z * ny)
        cz = quotient(rest, ny)
        return cx - box * wx, cz - slab * wz, rest - cz * ny

    def hot(n, at):
        return jnp.where(iota((n, pts), 0) == at, 1.0, 0.0).astype(BF16)

    tall_x, tall_z = wx + 2 * MARGIN, wz + 2 * MARGIN
    px, pz, py = where_is(face_x)
    row_x[...] = hot(tall_z, jnp.where((px >= 0) & (px < wx), pz + MARGIN, -1))
    hot_x[...] = hot(ny, py)
    px, pz, py = where_is(jnp.where(slab == 0, 2, 3))
    row_z[...] = hot(tall_x, jnp.where((pz >= 0) & (pz < wz), px + MARGIN, -1))
    hot_z[...] = hot(ny, py)
    for face, row_hot, hot_at in ((4, row_low, hot_low), (5, row_high, hot_high)):
        px, pz, py = where_is(face)
        row_hot[...] = hot(tall_z, pz + MARGIN)
        hot_at[...] = hot(WIDE, px + MARGIN)

    for a in range(2):
        @pl.when(hears_box[a])
        def _(a=a):
            for c in x_copies(a, given):
                c.wait_recv()
    for a in range(2):
        plane = edge_x[1 - a]
        for m in range(members):
            rows = pl.ds((m * wx + plane) * wz, wz)
            ghost = jnp.where(hears_box[a], xghost[a, m], 0.0)
            one[rows, :] = psend[1 - a, m] + coef[rows, :] * ghost
    for b in range(2):
        @pl.when(hears_slab[b])
        def _(b=b):
            z_copy(b, 0).wait_recv()
            row = edge_z[1 - b]
            for m in range(members):
                for x in range(wx):
                    at = pl.ds((m * wx + x) * wz + row, 1)
                    one[at, :] += coef[at, :] * zghost[b, m, x : x + 1, :]

    for a in range(2):
        for b in range(2):
            @pl.when(hears_box[a] & hears_slab[b])
            def _(a=a, b=b):
                corner_copy(a, b).wait_recv()
    for b in range(2):
        @pl.when(hears_slab[b])
        def _(b=b):
            z_copy(b, 1).wait_recv()
    for a in range(2):
        @pl.when(hears_box[a])
        def _(a=a):
            x_copies(a, parts)[0].wait_recv()

    def across(a, b, m):
        return jnp.where(hears_box[a] & hears_slab[b], corner[a, b, m : m + 1, :], 0.0)

    for a in range(2):
        for m in range(members):
            beside = now[pl.ds((m * wx + edge_x[1 - a]) * wz, wz), :]
            beside = beside + jnp.where(z_at == 0, across(a, 0, m), 0.0)
            beside = beside + jnp.where(z_at == wz - 1, across(a, 1, m), 0.0)
            xout[a, m] = jnp.where(hears_box[a], xpart[a, m] + xcour[a] * gains[m] * beside, 0.0)
    for b in range(2):
        for m in range(members):
            beside = zsend[1 - b, m]
            beside = beside + jnp.where(x_at == 0, across(0, b, m), 0.0)
            beside = beside + jnp.where(x_at == wx - 1, across(1, b, m), 0.0)
            zout[b, m] = jnp.where(hears_slab[b], zpart[b, m] + zghost[b, members] * gains_beyond[m][b] * beside, 0.0)

    for d in range(1, n_slab):
        give(d, 0).wait_recv()

    @pl.when(box_edge)
    def _():
        for d in range(1, n_slab):
            give(d, 1).wait_recv()

    @pl.when(slab_edge)
    def _():
        for d in range(1, n_slab):
            give(d, 2).wait_recv()

    values_y, values_x, values_z = ysend[...], xvsend[...], zvsend[jnp.where(slab == 0, 0, 1)]
    for d in range(1, n_slab):
        values_y = values_y + yrecv[d - 1]
        values_x = values_x + xvrecv[d - 1]
        values_z = values_z + zvrecv[d - 1]
    values_x = jnp.where(box_edge, values_x, 0.0)
    values_z = jnp.where(slab_edge, values_z, 0.0)

    def rows_of(v, k):
        return [v[k + t : k + t + 1] for t in both]

    low_y = place(row_low, rows_of(values_y, 0), hot_low)
    high_y = place(row_high, rows_of(values_y, steps), hot_high)
    on_z = place(row_z, rows_of(values_z, 0), hot_z)
    on_x = place(row_x, rows_of(values_x, 0), hot_x)
    plane_x = jnp.where(box == 0, 0, wx - 1)
    line_z = jnp.where(slab == 0, 0, wz - 1)
    tiles = ny // 128

    def source(t, x, k, first, count):
        rows = slice(first + MARGIN, first + MARGIN + count)
        lanes = slice(k * 128, (k + 1) * 128)
        at = x + MARGIN
        lane = iota((count, 128), 1)
        out = jnp.where(iota((count, 128), 0) + first == line_z, on_z[t][at : at + 1, lanes], 0.0)
        if k == 0:
            out = out + jnp.where(lane == 0, low_y[t][rows, at : at + 1], 0.0)
        if k == tiles - 1:
            out = out + jnp.where(lane == 127, high_y[t][rows, at : at + 1], 0.0)
        if x in (0, wx - 1):
            out = out + jnp.where(plane_x == x, on_x[t][rows, lanes], 0.0)
        return out

    for k in range(tiles):
        lanes = slice(k * 128, (k + 1) * 128)
        for x in range(wx):
            plane = source(0, x, k, -MARGIN, tall_z)
            for b, row in ((0, MARGIN - 1), (1, MARGIN + wz)):
                line = plane[row : row + 1]
                for m in range(members):
                    zout[b, m, x : x + 1, lanes] += line
            for m in range(members):
                one[pl.ds((m * wx + x) * wz, wz), lanes] += plane[MARGIN : MARGIN + wz]
            src[pl.ds(x * wz, wz), lanes] = source(1, x, k, 0, wz)
        for a, x in ((0, -1), (1, wx)):
            plane = source(0, x, k, 0, wz)
            for m in range(members):
                xout[a, m, :, lanes] += plane

    for a in range(2):
        @pl.when(sends_box[a])
        def _(a=a):
            for c in x_copies(a, (*given, *parts)):
                c.wait_send()
            for b in range(2):
                @pl.when(sends_slab[b])
                def _(b=b):
                    corner_copy(a, b).wait_send()
    for b in range(2):
        @pl.when(sends_slab[b])
        def _(b=b):
            for i in range(2):
                z_copy(b, i).wait_send()
    each_give(lambda c: c.wait_send())


def last_kernel(dims, one, now, coef, xout, zout, src, next_h, last_h, two, sem):
    members, wx, wz, ny = dims[:4]
    group = 4 if wx % 4 == 0 else 1
    parts = wx // group
    last = pltpu.make_async_copy(one, last_h, sem.at[members * parts])
    last.start()
    z_at, y_at = iota((wz, ny), 0), iota((wz, ny), 1)

    def put(m, g):
        rows = pl.ds((m * wx + g * group) * wz, group * wz)
        return pltpu.make_async_copy(two.at[rows], next_h.at[rows], sem.at[m * parts + g])

    for m in range(members):
        for x in range(wx):
            at = (m * wx + x) * wz
            rows = pl.ds(at, wz)
            c = one[rows, :]
            lap = along_y(c, y_at) - 6.0 * c
            lap = lap + (one[pl.ds(at - wz, wz), :] if x > 0 else xout[0, m])
            lap = lap + (one[pl.ds(at + wz, wz), :] if x < wx - 1 else xout[1, m])
            lap = lap + jnp.where(z_at == 0, zout[0, m, x : x + 1, :], pltpu.roll(c, 1, 0))
            lap = lap + jnp.where(z_at == wz - 1, zout[1, m, x : x + 1, :], pltpu.roll(c, wz - 1, 0))
            two[rows, :] = (2.0 * c - now[rows, :]) + coef[rows, :] * lap + src[pl.ds(x * wz, wz), :]
            if x % group == group - 1:
                put(m, x // group).start()
    last.wait()
    for m in range(members):
        for g in range(parts):
            put(m, g).wait()


def on_device(pressure_now, pressure_prev, courant_sq, member_profiles, member_ids, stored_slabs,
              slab_home, interp_weights, surface_cells):
    members, wx, wz, ny = pressure_now.shape
    slots, length, points = stored_slabs.shape
    pts = surface_cells.shape[1]
    n_box, n_slab = lax.axis_size("box"), lax.axis_size("slab")
    dims = (members, wx, wz, ny, slots, length, pts, n_box, n_slab)
    rows = members * wx * wz
    peers = n_slab - 1
    tall_x, tall_z = wx + 2 * MARGIN, wz + 2 * MARGIN
    vmem = pl.BlockSpec(memory_space=pltpu.VMEM)
    in_hbm = lambda a: pltpu.with_memory_space_constraint(a, pltpu.HBM)
    hbm = pl.BlockSpec(memory_space=pltpu.HBM)
    struct = lambda *shape: jax.ShapeDtypeStruct(shape, F32)
    f32 = lambda *shape: pltpu.VMEM(shape, F32)
    bf16 = lambda *shape: pltpu.VMEM(shape, BF16)
    dma = pltpu.SemaphoreType.DMA
    kept = pl.pallas_call(
        functools.partial(kernel, dims),
        out_shape=(struct(rows, ny), struct(rows, ny), struct(rows, ny),
                   struct(2, members, wz, ny), struct(2, members, wx, ny), struct(wx * wz, ny)),
        in_specs=[pl.BlockSpec(memory_space=pltpu.SMEM)] + [hbm] * 8,
        out_specs=(vmem,) * 6,
        scratch_shapes=[
            pltpu.SMEM(member_ids.shape, I32),
            pltpu.VMEM(member_profiles.shape, F32), pltpu.VMEM(interp_weights.shape, F32),
            pltpu.VMEM(surface_cells.shape, I32),
            f32(rows, ny), f32(wx * wz, ny),
            f32(slots * length, 2 * pts), f32(slots * length, 2 * pts), f32(slots * length, pts),
            f32(2, members, wz, ny), f32(2, members + 1, wx, ny), f32(2, members, wx, ny), f32(2, 2, members, ny),
            f32(2, members, wz, ny), f32(2, wz, ny), f32(2, members, wz, ny),
            f32(2, members + 1, wx, ny), f32(2, members, wx, ny), f32(2, 2, members, ny),
            bf16(tall_z, pts), bf16(tall_x, pts), bf16(tall_z, pts), bf16(tall_z, pts),
            bf16(ny, pts), bf16(ny, pts), bf16(WIDE, pts), bf16(WIDE, pts),
            f32(4, pts), f32(2, pts), f32(2, 2, pts),
            f32(peers, 4, pts), f32(peers, 2, pts), f32(peers, 2, pts),
            dma((10,)), dma((4, members + 2)), dma((4, members + 2)), dma((2, 2)), dma((2, 2)),
            dma((peers, 3)), dma((peers, 3)), pltpu.SemaphoreType.REGULAR((2,)),
        ],
        compiler_params=pltpu.CompilerParams(collective_id=0, has_side_effects=True,
                                             vmem_limit_bytes=32 * 1024 * 1024),
    )(slab_home, *(in_hbm(a) for a in (
        member_ids, member_profiles, interp_weights, surface_cells,
        pressure_now.reshape(rows, ny), pressure_prev.reshape(rows, ny),
        courant_sq.reshape(wx * wz, ny), stored_slabs.reshape(slots * length, points),
    )))
    placed = pltpu.HBM((rows, ny), F32)
    new, last = pl.pallas_call(
        functools.partial(last_kernel, dims),
        out_shape=(placed, placed),
        in_specs=[vmem] * 6,
        out_specs=(hbm, hbm),
        scratch_shapes=[f32(rows, ny), dma((members * wx + 1,))],
        compiler_params=pltpu.CompilerParams(vmem_limit_bytes=4 * 1024 * 1024),
    )(*kept)
    return new.reshape(pressure_now.shape), last.reshape(pressure_now.shape)


def solution(mesh):
    in_specs = (
        P("ens", "box", "slab", None), P("ens", "box", "slab", None), P("box", "slab", None), P(),
        P("ens"), P("slab", None, None), P("ens"), P(), P(),
    )
    out_specs = (P("ens", "box", "slab", None), P("ens", "box", "slab", None))
    return jax.shard_map(on_device, mesh=mesh, in_specs=in_specs, out_specs=out_specs, check_vma=False)
```

```python
import functools

import jax
import jax.numpy as jnp
from jax import lax
from jax.experimental import pallas as pl
from jax.experimental.pallas import tpu as pltpu
from jax.sharding import PartitionSpec as P

F32, BF16, I32 = jnp.float32, jnp.bfloat16, jnp.int32
MESH = pl.DeviceIdType.MESH
MARGIN, WIDE = 8, 128


def iota(shape, dim):
    return lax.broadcasted_iota(I32, shape, dim)


def quotient(values, divisor):
    if divisor & (divisor - 1) == 0:
        return lax.shift_right_logical(values, divisor.bit_length() - 1)
    return lax.div(values, jnp.full_like(values, divisor))


def split2(v):
    high = v.astype(BF16).astype(F32)
    return high, v - high


def place(row_hot, values, right):
    rows = row_hot.shape[0]
    parts = []
    for v in values:
        for term in split2(v):
            wide = jnp.broadcast_to(term, (16, v.shape[1])).astype(BF16)
            parts += [row_hot[r : r + 16, :] * wide for r in range(0, rows, 16)]
    left = jnp.concatenate(parts, axis=0)
    sums = lax.dot_general(left, right[...], (((1,), (1,)), ((), ())), preferred_element_type=F32)
    return [sums[2 * t * rows : (2 * t + 1) * rows] + sums[(2 * t + 1) * rows : (2 * t + 2) * rows]
            for t in range(len(values))]


def along_y(c, y_at):
    ny = c.shape[1]
    return (jnp.where(y_at == 0, 0.0, pltpu.roll(c, 1, 1))
            + jnp.where(y_at == ny - 1, 0.0, pltpu.roll(c, ny - 1, 1)))


def kernel(dims, home, ids_h, prof_h, weights_h, cells_h, now_h, prev_h, cour_h, slabs_h,
           one, now, coef, xout, zout, src,
           ids, prof, weights, cells, prev, cour, slab_y, slab_z, slab_x,
           psend, zsend, zpsend, csend, xghost, xcour, xpart, zghost, zpart, corner,
           row_x, row_z, row_low, row_high, hot_x, hot_z, hot_low, hot_high,
           ysend, xvsend, zvsend, yrecv, xvrecv, zvrecv,
           load_sem, hs_sem, hr_sem, cs_sem, cr_sem, vs_sem, vr_sem, diag_sem):
    members, wx, wz, ny, slots, length, pts, n_box, n_slab = dims
    steps = 2
    block = wx * wz
    box, slab = lax.axis_index("box"), lax.axis_index("slab")
    face_x = jnp.where(box == 0, 0, 1)
    box_edge = (box == 0) | (box == n_box - 1)
    slab_edge = (slab == 0) | (slab == n_slab - 1)
    pairs = (
        (slabs_h.at[:, pl.ds(4 * pts, 2 * pts)], slab_y), (weights_h, weights),
        (slabs_h.at[:, pl.ds(2 * pts, 2 * pts)], slab_z),
        (slabs_h.at[:, pl.ds(pl.multiple_of(face_x * pts, 128), pts)], slab_x),
        (now_h, now), (cour_h, cour), (prof_h, prof), (ids_h, ids), (prev_h, prev), (cells_h, cells))
    loads = [pltpu.make_async_copy(src_, dst, load_sem.at[i]) for i, (src_, dst) in enumerate(pairs)]

    barrier = pltpu.get_barrier_semaphore()

    def greet(target):
        pl.semaphore_signal(barrier, inc=1, device_id=target, device_id_type=MESH)

    sends_box = (box < n_box - 1, box > 0)
    sends_slab = (slab < n_slab - 1, slab > 0)
    hears_box = (box > 0, box < n_box - 1)
    hears_slab = (slab > 0, slab < n_slab - 1)
    shift = (1, -1)

    for d in range(1, n_slab):
        greet({"slab": lax.rem(slab + d, n_slab)})
    for a in range(2):
        @pl.when(sends_box[a])
        def _(a=a):
            greet({"box": box + shift[a]})
    for c in loads:
        c.start()

    for i in range(4):
        loads[i].wait()
    eye = iota((length, length), 0) == iota((length, length), 1)
    cols = []
    for t in range(steps):
        col = jnp.sum(jnp.where(eye, weights[t : t + 1, :], 0.0), axis=1, keepdims=True)
        cols.append([jnp.where(home[0] == slab * slots + s, col, 0.0) for s in range(slots)])

    def offered(ref, at, t):
        where = pl.ds(at, pts)
        total = cols[t][0] * ref[pl.ds(0, length), where]
        for s in range(1, slots):
            total = total + cols[t][s] * ref[pl.ds(s * length, length), where]
        return jnp.sum(total, axis=0, keepdims=True)

    both = range(steps)
    ysend[...] = jnp.concatenate([offered(slab_y, f * pts, t) for f in range(2) for t in both], axis=0)
    for f in range(2):
        zvsend[f] = jnp.concatenate([offered(slab_z, f * pts, t) for t in both], axis=0)
    xvsend[...] = jnp.concatenate([offered(slab_x, 0, t) for t in both], axis=0)

    loads[4].wait()
    loads[5].wait()
    edge_x, edge_z = (wx - 1, 0), (wz - 1, 0)
    for b in range(2):
        for x in range(wx):
            for m in range(members):
                zsend[b, m, x : x + 1, :] = now[pl.ds((m * wx + x) * wz + edge_z[b], 1), :]
            zsend[b, members, x : x + 1, :] = cour[pl.ds(x * wz + edge_z[b], 1), :]
        for a in range(2):
            for m in range(members):
                csend[a, b, m : m + 1, :] = now[pl.ds((m * wx + edge_x[a]) * wz + edge_z[b], 1), :]

    def give(d, kind):
        peer = lax.rem(slab + d, n_slab)
        ref, into = ((ysend, yrecv), (xvsend, xvrecv), (zvsend.at[0], zvrecv), (zvsend.at[1], zvrecv))[kind]
        k = min(kind, 2)
        return pltpu.make_async_remote_copy(
            ref, into.at[d - 1], vs_sem.at[d - 1, k], vr_sem.at[d - 1, k],
            device_id={"slab": peer}, device_id_type=MESH)

    def gives(d, kind):
        peer = lax.rem(slab + d, n_slab)
        return (None, box_edge, peer == 0, peer == n_slab - 1)[kind]

    def each_give(act):
        for d in range(1, n_slab):
            for kind in range(4):
                cond = gives(d, kind)
                if cond is None:
                    act(give(d, kind))
                else:
                    @pl.when(cond)
                    def _(d=d, kind=kind):
                        act(give(d, kind))

    given, parts = range(members + 1), range(members + 1, members + 2)

    def x_copies(a, which):
        peer = {"box": box + shift[a]}
        refs = [(now.at[pl.ds((m * wx + edge_x[a]) * wz, wz)], xghost.at[a, m]) for m in range(members)]
        refs += [(cour.at[pl.ds(edge_x[a] * wz, wz)], xcour.at[a]), (psend.at[a], xpart.at[a])]
        return [pltpu.make_async_remote_copy(*refs[i], hs_sem.at[a, i], hr_sem.at[a, i], device_id=peer, device_id_type=MESH)
                for i in which]

    def z_copy(b, i):
        source_, target = ((zsend.at[b], zghost.at[b]), (zpsend.at[b], zpart.at[b]))[i]
        return pltpu.make_async_remote_copy(source_, target, hs_sem.at[2 + b, i], hr_sem.at[2 + b, i],
                                            device_id={"slab": slab + shift[b]}, device_id_type=MESH)

    def corner_copy(a, b):
        return pltpu.make_async_remote_copy(
            csend.at[a, b], corner.at[a, b], cs_sem.at[a, b], cr_sem.at[a, b],
            device_id={"box": box + shift[a], "slab": slab + shift[b]}, device_id_type=MESH)

    def send_corners(a):
        @pl.when(sends_box[a])
        def _():
            pl.semaphore_wait(diag_sem.at[1 - a], 1)
            for b in range(2):
                @pl.when(sends_slab[b])
                def _(b=b):
                    corner_copy(a, b).start()

    box_peers = jnp.where(box > 0, 1, 0) + jnp.where(box < n_box - 1, 1, 0)
    pl.semaphore_wait(barrier, n_slab - 1 + box_peers)
    for a in range(2):
        @pl.when(sends_box[a])
        def _(a=a):
            pl.semaphore_signal(diag_sem.at[a], inc=1, device_id={"box": box + shift[a]}, device_id_type=MESH)
            for c in x_copies(a, given):
                c.start()
    each_give(lambda c: c.start())
    for b in range(2):
        @pl.when(sends_slab[b])
        def _(b=b):
            z_copy(b, 0).start()

    loads[6].wait()
    loads[7].wait()
    bank, total_z = prof.shape
    here = iota((wz, total_z), 1) == slab * wz + iota((wz, total_z), 0)
    beyond = [iota((1, total_z), 1) == slab * wz + at for at in (-1, wz)]
    gains, gains_beyond = [], []
    for m in range(members):
        mine = jnp.sum(jnp.where(iota((bank, total_z), 0) == ids[m], prof[...], 0.0), axis=0, keepdims=True)
        gains.append(1.0 + jnp.sum(jnp.where(here, mine, 0.0), axis=1, keepdims=True))
        gains_beyond.append([1.0 + jnp.sum(jnp.where(at, mine, 0.0), axis=1, keepdims=True) for at in beyond])

    loads[8].wait()
    z_at, y_at, x_at = iota((wz, ny), 0), iota((wz, ny), 1), iota((wx, ny), 0)
    for m in range(members):
        for x in (0, wx - 1, *range(1, wx - 1)):
            at = (m * wx + x) * wz
            rows = pl.ds(at, wz)
            c = now[rows, :]
            k = cour[pl.ds(x * wz, wz), :] * gains[m]
            coef[rows, :] = k
            lap = along_y(c, y_at) - 6.0 * c
            if x > 0:
                lap = lap + now[pl.ds(at - wz, wz), :]
            if x < wx - 1:
                lap = lap + now[pl.ds(at + wz, wz), :]
            lap = lap + jnp.where(z_at == 0, 0.0, pltpu.roll(c, 1, 0))
            lap = lap + jnp.where(z_at == wz - 1, 0.0, pltpu.roll(c, wz - 1, 0))
            nxt = (2.0 * c - prev[rows, :]) + k * lap
            if x == wx - 1:
                psend[0, m] = nxt
            elif x == 0:
                psend[1, m] = nxt
            else:
                one[rows, :] = nxt
            for b in range(2):
                zpsend[b, m, x : x + 1, :] = nxt[edge_z[b] : edge_z[b] + 1, :]
    send_corners(1)
    for a in range(2):
        @pl.when(sends_box[a])
        def _(a=a):
            x_copies(a, parts)[0].start()
    for b in range(2):
        @pl.when(sends_slab[b])
        def _(b=b):
            z_copy(b, 1).start()

    loads[9].wait()

    def where_is(face):
        cell = cells[pl.ds(face, 1), :]
        cx = quotient(cell, total_z * ny)
        rest = cell - cx * (total_z * ny)
        cz = quotient(rest, ny)
        return cx - box * wx, cz - slab * wz, rest - cz * ny

    def hot(n, at):
        return jnp.where(iota((n, pts), 0) == at, 1.0, 0.0).astype(BF16)

    tall_x, tall_z = wx + 2 * MARGIN, wz + 2 * MARGIN
    px, pz, py = where_is(face_x)
    row_x[...] = hot(tall_z, jnp.where((px >= 0) & (px < wx), pz + MARGIN, -1))
    hot_x[...] = hot(ny, py)
    px, pz, py = where_is(jnp.where(slab == 0, 2, 3))
    row_z[...] = hot(tall_x, jnp.where((pz >= 0) & (pz < wz), px + MARGIN, -1))
    hot_z[...] = hot(ny, py)
    for face, row_hot, hot_at in ((4, row_low, hot_low), (5, row_high, hot_high)):
        px, pz, py = where_is(face)
        row_hot[...] = hot(tall_z, pz + MARGIN)
        hot_at[...] = hot(WIDE, px + MARGIN)

    send_corners(0)


    for d in range(1, n_slab):
        give(d, 0).wait_recv()

    @pl.when(box_edge)
    def _():
        for d in range(1, n_slab):
            give(d, 1).wait_recv()

    @pl.when(slab_edge)
    def _():
        for d in range(1, n_slab):
            give(d, 2).wait_recv()

    values_y, values_x, values_z = ysend[...], xvsend[...], zvsend[jnp.where(slab == 0, 0, 1)]
    for d in range(1, n_slab):
        values_y = values_y + yrecv[d - 1]
        values_x = values_x + xvrecv[d - 1]
        values_z = values_z + zvrecv[d - 1]
    values_x = jnp.where(box_edge, values_x, 0.0)
    values_z = jnp.where(slab_edge, values_z, 0.0)

    def rows_of(v, k):
        return [v[k + t : k + t + 1] for t in both]

    low_y = place(row_low, rows_of(values_y, 0), hot_low)
    high_y = place(row_high, rows_of(values_y, steps), hot_high)
    on_z = place(row_z, rows_of(values_z, 0), hot_z)
    on_x = place(row_x, rows_of(values_x, 0), hot_x)
    for a in range(2):
        @pl.when(hears_box[a])
        def _(a=a):
            for c in x_copies(a, given):
                c.wait_recv()
    for a in range(2):
        plane = edge_x[1 - a]
        for m in range(members):
            rows = pl.ds((m * wx + plane) * wz, wz)
            ghost = jnp.where(hears_box[a], xghost[a, m], 0.0)
            one[rows, :] = psend[1 - a, m] + coef[rows, :] * ghost
    for b in range(2):
        @pl.when(hears_slab[b])
        def _(b=b):
            z_copy(b, 0).wait_recv()
            row = edge_z[1 - b]
            for m in range(members):
                for x in range(wx):
                    at = pl.ds((m * wx + x) * wz + row, 1)
                    one[at, :] += coef[at, :] * zghost[b, m, x : x + 1, :]

    for a in range(2):
        for b in range(2):
            @pl.when(hears_box[a] & hears_slab[b])
            def _(a=a, b=b):
                corner_copy(a, b).wait_recv()
    for b in range(2):
        @pl.when(hears_slab[b])
        def _(b=b):
            z_copy(b, 1).wait_recv()
    for a in range(2):
        @pl.when(hears_box[a])
        def _(a=a):
            x_copies(a, parts)[0].wait_recv()

    def across(a, b, m):
        return jnp.where(hears_box[a] & hears_slab[b], corner[a, b, m : m + 1, :], 0.0)

    for a in range(2):
        for m in range(members):
            beside = now[pl.ds((m * wx + edge_x[1 - a]) * wz, wz), :]
            beside = beside + jnp.where(z_at == 0, across(a, 0, m), 0.0)
            beside = beside + jnp.where(z_at == wz - 1, across(a, 1, m), 0.0)
            xout[a, m] = jnp.where(hears_box[a], xpart[a, m] + xcour[a] * gains[m] * beside, 0.0)
    for b in range(2):
        for m in range(members):
            beside = zsend[1 - b, m]
            beside = beside + jnp.where(x_at == 0, across(0, b, m), 0.0)
            beside = beside + jnp.where(x_at == wx - 1, across(1, b, m), 0.0)
            zout[b, m] = jnp.where(hears_slab[b], zpart[b, m] + zghost[b, members] * gains_beyond[m][b] * beside, 0.0)

    plane_x = jnp.where(box == 0, 0, wx - 1)
    line_z = jnp.where(slab == 0, 0, wz - 1)
    tiles = ny // 128

    def source(t, x, k, first, count):
        rows = slice(first + MARGIN, first + MARGIN + count)
        lanes = slice(k * 128, (k + 1) * 128)
        at = x + MARGIN
        lane = iota((count, 128), 1)
        out = jnp.where(iota((count, 128), 0) + first == line_z, on_z[t][at : at + 1, lanes], 0.0)
        if k == 0:
            out = out + jnp.where(lane == 0, low_y[t][rows, at : at + 1], 0.0)
        if k == tiles - 1:
            out = out + jnp.where(lane == 127, high_y[t][rows, at : at + 1], 0.0)
        if x in (0, wx - 1):
            out = out + jnp.where(plane_x == x, on_x[t][rows, lanes], 0.0)
        return out

    for k in range(tiles):
        lanes = slice(k * 128, (k + 1) * 128)
        for x in range(wx):
            plane = source(0, x, k, -MARGIN, tall_z)
            for b, row in ((0, MARGIN - 1), (1, MARGIN + wz)):
                line = plane[row : row + 1]
                for m in range(members):
                    zout[b, m, x : x + 1, lanes] += line
            for m in range(members):
                one[pl.ds((m * wx + x) * wz, wz), lanes] += plane[MARGIN : MARGIN + wz]
            src[pl.ds(x * wz, wz), lanes] = source(1, x, k, 0, wz)
        for a, x in ((0, -1), (1, wx)):
            plane = source(0, x, k, 0, wz)
            for m in range(members):
                xout[a, m, :, lanes] += plane

    for a in range(2):
        @pl.when(sends_box[a])
        def _(a=a):
            for c in x_copies(a, (*given, *parts)):
                c.wait_send()
            for b in range(2):
                @pl.when(sends_slab[b])
                def _(b=b):
                    corner_copy(a, b).wait_send()
    for b in range(2):
        @pl.when(sends_slab[b])
        def _(b=b):
            for i in range(2):
                z_copy(b, i).wait_send()
    each_give(lambda c: c.wait_send())


def last_kernel(dims, one, now, coef, xout, zout, src, next_h, last_h, two, sem):
    members, wx, wz, ny = dims[:4]
    group = 4 if wx % 4 == 0 else 1
    parts = wx // group
    last = pltpu.make_async_copy(one, last_h, sem.at[members * parts])
    last.start()
    z_at, y_at = iota((wz, ny), 0), iota((wz, ny), 1)

    def put(m, g):
        rows = pl.ds((m * wx + g * group) * wz, group * wz)
        return pltpu.make_async_copy(two.at[rows], next_h.at[rows], sem.at[m * parts + g])

    for m in range(members):
        for x in range(wx):
            at = (m * wx + x) * wz
            rows = pl.ds(at, wz)
            c = one[rows, :]
            lap = along_y(c, y_at) - 6.0 * c
            lap = lap + (one[pl.ds(at - wz, wz), :] if x > 0 else xout[0, m])
            lap = lap + (one[pl.ds(at + wz, wz), :] if x < wx - 1 else xout[1, m])
            lap = lap + jnp.where(z_at == 0, zout[0, m, x : x + 1, :], pltpu.roll(c, 1, 0))
            lap = lap + jnp.where(z_at == wz - 1, zout[1, m, x : x + 1, :], pltpu.roll(c, wz - 1, 0))
            two[rows, :] = (2.0 * c - now[rows, :]) + coef[rows, :] * lap + src[pl.ds(x * wz, wz), :]
            if x % group == group - 1:
                put(m, x // group).start()
    last.wait()
    for m in range(members):
        for g in range(parts):
            put(m, g).wait()


def on_device(pressure_now, pressure_prev, courant_sq, member_profiles, member_ids, stored_slabs,
              slab_home, interp_weights, surface_cells):
    members, wx, wz, ny = pressure_now.shape
    slots, length, points = stored_slabs.shape
    pts = surface_cells.shape[1]
    n_box, n_slab = lax.axis_size("box"), lax.axis_size("slab")
    dims = (members, wx, wz, ny, slots, length, pts, n_box, n_slab)
    rows = members * wx * wz
    peers = n_slab - 1
    tall_x, tall_z = wx + 2 * MARGIN, wz + 2 * MARGIN
    vmem = pl.BlockSpec(memory_space=pltpu.VMEM)
    in_hbm = lambda a: pltpu.with_memory_space_constraint(a, pltpu.HBM)
    hbm = pl.BlockSpec(memory_space=pltpu.HBM)
    struct = lambda *shape: jax.ShapeDtypeStruct(shape, F32)
    f32 = lambda *shape: pltpu.VMEM(shape, F32)
    bf16 = lambda *shape: pltpu.VMEM(shape, BF16)
    dma = pltpu.SemaphoreType.DMA
    kept = pl.pallas_call(
        functools.partial(kernel, dims),
        out_shape=(struct(rows, ny), struct(rows, ny), struct(rows, ny),
                   struct(2, members, wz, ny), struct(2, members, wx, ny), struct(wx * wz, ny)),
        in_specs=[pl.BlockSpec(memory_space=pltpu.SMEM)] + [hbm] * 8,
        out_specs=(vmem,) * 6,
        scratch_shapes=[
            pltpu.SMEM(member_ids.shape, I32),
            pltpu.VMEM(member_profiles.shape, F32), pltpu.VMEM(interp_weights.shape, F32),
            pltpu.VMEM(surface_cells.shape, I32),
            f32(rows, ny), f32(wx * wz, ny),
            f32(slots * length, 2 * pts), f32(slots * length, 2 * pts), f32(slots * length, pts),
            f32(2, members, wz, ny), f32(2, members + 1, wx, ny), f32(2, members, wx, ny), f32(2, 2, members, ny),
            f32(2, members, wz, ny), f32(2, wz, ny), f32(2, members, wz, ny),
            f32(2, members + 1, wx, ny), f32(2, members, wx, ny), f32(2, 2, members, ny),
            bf16(tall_z, pts), bf16(tall_x, pts), bf16(tall_z, pts), bf16(tall_z, pts),
            bf16(ny, pts), bf16(ny, pts), bf16(WIDE, pts), bf16(WIDE, pts),
            f32(4, pts), f32(2, pts), f32(2, 2, pts),
            f32(peers, 4, pts), f32(peers, 2, pts), f32(peers, 2, pts),
            dma((10,)), dma((4, members + 2)), dma((4, members + 2)), dma((2, 2)), dma((2, 2)),
            dma((peers, 3)), dma((peers, 3)), pltpu.SemaphoreType.REGULAR((2,)),
        ],
        compiler_params=pltpu.CompilerParams(collective_id=0, has_side_effects=True,
                                             vmem_limit_bytes=32 * 1024 * 1024),
    )(slab_home, *(in_hbm(a) for a in (
        member_ids, member_profiles, interp_weights, surface_cells,
        pressure_now.reshape(rows, ny), pressure_prev.reshape(rows, ny),
        courant_sq.reshape(wx * wz, ny), stored_slabs.reshape(slots * length, points),
    )))
    placed = pltpu.HBM((rows, ny), F32)
    new, last = pl.pallas_call(
        functools.partial(last_kernel, dims),
        out_shape=(placed, placed),
        in_specs=[vmem] * 6,
        out_specs=(hbm, hbm),
        scratch_shapes=[f32(rows, ny), dma((members * wx + 1,))],
        compiler_params=pltpu.CompilerParams(vmem_limit_bytes=4 * 1024 * 1024),
    )(*kept)
    return new.reshape(pressure_now.shape), last.reshape(pressure_now.shape)


def solution(mesh):
    in_specs = (
        P("ens", "box", "slab", None), P("ens", "box", "slab", None), P("box", "slab", None), P(),
        P("ens"), P("slab", None, None), P("ens"), P(), P(),
    )
    out_specs = (P("ens", "box", "slab", None), P("ens", "box", "slab", None))
    return jax.shard_map(on_device, mesh=mesh, in_specs=in_specs, out_specs=out_specs, check_vma=False)
```

```python
import functools

import jax
import jax.numpy as jnp
from jax import lax
from jax.experimental import pallas as pl
from jax.experimental.pallas import tpu as pltpu
from jax.sharding import PartitionSpec as P

F32, BF16, I32 = jnp.float32, jnp.bfloat16, jnp.int32
MESH = pl.DeviceIdType.MESH
MARGIN, WIDE = 8, 128


def iota(shape, dim):
    return lax.broadcasted_iota(I32, shape, dim)


def quotient(values, divisor):
    if divisor & (divisor - 1) == 0:
        return lax.shift_right_logical(values, divisor.bit_length() - 1)
    return lax.div(values, jnp.full_like(values, divisor))


def split2(v):
    high = v.astype(BF16).astype(F32)
    return high, v - high


def place(row_hot, values, right):
    rows = row_hot.shape[0]
    parts = []
    for v in values:
        for term in split2(v):
            wide = jnp.broadcast_to(term, (16, v.shape[1])).astype(BF16)
            parts += [row_hot[r : r + 16, :] * wide for r in range(0, rows, 16)]
    left = jnp.concatenate(parts, axis=0)
    sums = lax.dot_general(left, right[...], (((1,), (1,)), ((), ())), preferred_element_type=F32)
    return [sums[2 * t * rows : (2 * t + 1) * rows] + sums[(2 * t + 1) * rows : (2 * t + 2) * rows]
            for t in range(len(values))]


def along_y(c, y_at):
    ny = c.shape[1]
    return (jnp.where(y_at == 0, 0.0, pltpu.roll(c, 1, 1))
            + jnp.where(y_at == ny - 1, 0.0, pltpu.roll(c, ny - 1, 1)))


def kernel(dims, home, ids_h, prof_h, weights_h, cells_h, now_h, prev_h, cour_h, slabs_h,
           one, now, coef, xout, zout, src,
           ids, prof, weights, cells, prev, cour, slab_y, slab_z, slab_x,
           psend, zsend, zpsend, csend, xghost, xcour, xpart, zghost, zpart, corner,
           row_x, row_z, row_low, row_high, hot_x, hot_z, hot_low, hot_high,
           ysend, xvsend, zvsend, yrecv, xvrecv, zvrecv,
           load_sem, hs_sem, hr_sem, cs_sem, cr_sem, vs_sem, vr_sem, here_sem, peer_sem):
    members, wx, wz, ny, slots, length, pts, n_box, n_slab = dims
    steps = 2
    block = wx * wz
    box, slab = lax.axis_index("box"), lax.axis_index("slab")
    face_x = jnp.where(box == 0, 0, 1)
    box_edge = (box == 0) | (box == n_box - 1)
    slab_edge = (slab == 0) | (slab == n_slab - 1)
    pairs = (
        (slabs_h.at[:, pl.ds(4 * pts, 2 * pts)], slab_y), (weights_h, weights),
        (slabs_h.at[:, pl.ds(2 * pts, 2 * pts)], slab_z),
        (slabs_h.at[:, pl.ds(pl.multiple_of(face_x * pts, 128), pts)], slab_x),
        (now_h, now), (cour_h, cour), (prof_h, prof), (ids_h, ids), (prev_h, prev), (cells_h, cells))
    loads = [pltpu.make_async_copy(src_, dst, load_sem.at[i]) for i, (src_, dst) in enumerate(pairs)]

    barrier = pltpu.get_barrier_semaphore()

    def greet(target):
        pl.semaphore_signal(barrier, inc=1, device_id=target, device_id_type=MESH)

    sends_box = (box < n_box - 1, box > 0)
    sends_slab = (slab < n_slab - 1, slab > 0)
    hears_box = (box > 0, box < n_box - 1)
    hears_slab = (slab > 0, slab < n_slab - 1)
    shift = (1, -1)

    @pl.when(sends_box[0])
    def _():
        greet({"box": box + 1})

    @pl.when(sends_box[0] & sends_slab[0])
    def _():
        greet({"box": box + 1, "slab": slab + 1})

    for d in range(1, n_slab):
        @pl.when(slab + d < n_slab)
        def _(d=d):
            greet({"slab": slab + d})
    for c in loads:
        c.start()
    lower_box = jnp.where(box > 0, 1, 0)

    @pl.when((box > 0) | (slab > 0))
    def _():
        pl.semaphore_wait(barrier, slab + lower_box * jnp.where(slab > 0, 2, 1))

    def tell(ref, target):
        pl.semaphore_signal(ref, inc=1, device_id=target, device_id_type=MESH)

    @pl.when(sends_box[1])
    def _():
        tell(here_sem.at[0], {"box": box - 1})

    for d in range(1, n_slab):
        @pl.when(slab >= d)
        def _(d=d):
            tell(peer_sem.at[d - 1], {"slab": slab - d})

    @pl.when(sends_box[1] & sends_slab[1])
    def _():
        tell(here_sem.at[1], {"box": box - 1, "slab": slab - 1})

    for i in range(4):
        loads[i].wait()
    eye = iota((length, length), 0) == iota((length, length), 1)
    cols = []
    for t in range(steps):
        col = jnp.sum(jnp.where(eye, weights[t : t + 1, :], 0.0), axis=1, keepdims=True)
        cols.append([jnp.where(home[0] == slab * slots + s, col, 0.0) for s in range(slots)])

    def offered(ref, at, t):
        where = pl.ds(at, pts)
        total = cols[t][0] * ref[pl.ds(0, length), where]
        for s in range(1, slots):
            total = total + cols[t][s] * ref[pl.ds(s * length, length), where]
        return jnp.sum(total, axis=0, keepdims=True)

    both = range(steps)
    ysend[...] = jnp.concatenate([offered(slab_y, f * pts, t) for f in range(2) for t in both], axis=0)
    for f in range(2):
        zvsend[f] = jnp.concatenate([offered(slab_z, f * pts, t) for t in both], axis=0)
    xvsend[...] = jnp.concatenate([offered(slab_x, 0, t) for t in both], axis=0)

    loads[4].wait()
    loads[5].wait()
    edge_x, edge_z = (wx - 1, 0), (wz - 1, 0)
    for b in range(2):
        for x in range(wx):
            for m in range(members):
                zsend[b, m, x : x + 1, :] = now[pl.ds((m * wx + x) * wz + edge_z[b], 1), :]
            zsend[b, members, x : x + 1, :] = cour[pl.ds(x * wz + edge_z[b], 1), :]
        for a in range(2):
            for m in range(members):
                csend[a, b, m : m + 1, :] = now[pl.ds((m * wx + edge_x[a]) * wz + edge_z[b], 1), :]

    def give(d, kind):
        peer = lax.rem(slab + d, n_slab)
        ref, into = ((ysend, yrecv), (xvsend, xvrecv), (zvsend.at[0], zvrecv), (zvsend.at[1], zvrecv))[kind]
        k = min(kind, 2)
        return pltpu.make_async_remote_copy(
            ref, into.at[d - 1], vs_sem.at[d - 1, k], vr_sem.at[d - 1, k],
            device_id={"slab": peer}, device_id_type=MESH)

    def gives(d, kind):
        peer = lax.rem(slab + d, n_slab)
        return (None, box_edge, peer == 0, peer == n_slab - 1)[kind]

    given, parts = range(members + 1), range(members + 1, members + 2)

    def x_copies(a, which):
        peer = {"box": box + shift[a]}
        refs = [(now.at[pl.ds((m * wx + edge_x[a]) * wz, wz)], xghost.at[a, m]) for m in range(members)]
        refs += [(cour.at[pl.ds(edge_x[a] * wz, wz)], xcour.at[a]), (psend.at[a], xpart.at[a])]
        return [pltpu.make_async_remote_copy(*refs[i], hs_sem.at[a, i], hr_sem.at[a, i], device_id=peer, device_id_type=MESH)
                for i in which]

    def z_copy(b, i):
        source_, target = ((zsend.at[b], zghost.at[b]), (zpsend.at[b], zpart.at[b]))[i]
        return pltpu.make_async_remote_copy(source_, target, hs_sem.at[2 + b, i], hr_sem.at[2 + b, i],
                                            device_id={"slab": slab + shift[b]}, device_id_type=MESH)

    def corner_copy(a, b):
        return pltpu.make_async_remote_copy(
            csend.at[a, b], corner.at[a, b], cs_sem.at[a, b], cr_sem.at[a, b],
            device_id={"box": box + shift[a], "slab": slab + shift[b]}, device_id_type=MESH)

    def give_all(d, act):
        for kind in range(4):
            cond = gives(d, kind)
            if cond is None:
                act(give(d, kind))
            else:
                @pl.when(cond)
                def _(kind=kind):
                    act(give(d, kind))

    for d in range(1, n_slab):
        @pl.when(slab + d >= n_slab)
        def _(d=d):
            give_all(d, lambda c: c.start())

    @pl.when(sends_box[1])
    def _():
        for c in x_copies(1, given):
            c.start()

    @pl.when(sends_slab[1])
    def _():
        z_copy(1, 0).start()

    @pl.when(sends_box[1] & sends_slab[1])
    def _():
        corner_copy(1, 1).start()

    loads[6].wait()
    loads[7].wait()
    bank, total_z = prof.shape
    here = iota((wz, total_z), 1) == slab * wz + iota((wz, total_z), 0)
    beyond = [iota((1, total_z), 1) == slab * wz + at for at in (-1, wz)]
    gains, gains_beyond = [], []
    for m in range(members):
        mine = jnp.sum(jnp.where(iota((bank, total_z), 0) == ids[m], prof[...], 0.0), axis=0, keepdims=True)
        gains.append(1.0 + jnp.sum(jnp.where(here, mine, 0.0), axis=1, keepdims=True))
        gains_beyond.append([1.0 + jnp.sum(jnp.where(at, mine, 0.0), axis=1, keepdims=True) for at in beyond])

    loads[8].wait()
    z_at, y_at, x_at = iota((wz, ny), 0), iota((wz, ny), 1), iota((wx, ny), 0)
    for m in range(members):
        for x in (0, wx - 1, *range(1, wx - 1)):
            at = (m * wx + x) * wz
            rows = pl.ds(at, wz)
            c = now[rows, :]
            k = cour[pl.ds(x * wz, wz), :] * gains[m]
            coef[rows, :] = k
            lap = along_y(c, y_at) - 6.0 * c
            if x > 0:
                lap = lap + now[pl.ds(at - wz, wz), :]
            if x < wx - 1:
                lap = lap + now[pl.ds(at + wz, wz), :]
            lap = lap + jnp.where(z_at == 0, 0.0, pltpu.roll(c, 1, 0))
            lap = lap + jnp.where(z_at == wz - 1, 0.0, pltpu.roll(c, wz - 1, 0))
            nxt = (2.0 * c - prev[rows, :]) + k * lap
            if x == wx - 1:
                psend[0, m] = nxt
            elif x == 0:
                psend[1, m] = nxt
            else:
                one[rows, :] = nxt
            for b in range(2):
                zpsend[b, m, x : x + 1, :] = nxt[edge_z[b] : edge_z[b] + 1, :]
    @pl.when(sends_box[1])
    def _():
        x_copies(1, parts)[0].start()

    @pl.when(sends_slab[1])
    def _():
        z_copy(1, 1).start()

    for d in range(1, n_slab):
        @pl.when(slab + d < n_slab)
        def _(d=d):
            pl.semaphore_wait(peer_sem.at[d - 1], 1)
            give_all(d, lambda c: c.start())
            if d == 1:
                for i in range(2):
                    z_copy(0, i).start()

                @pl.when(sends_box[1])
                def _():
                    corner_copy(1, 0).start()

    @pl.when(sends_box[0])
    def _():
        pl.semaphore_wait(here_sem.at[0], 1)
        for c in x_copies(0, (*given, *parts)):
            c.start()

        @pl.when(sends_slab[1])
        def _():
            corner_copy(0, 1).start()

    @pl.when(sends_box[0] & sends_slab[0])
    def _():
        pl.semaphore_wait(here_sem.at[1], 1)
        corner_copy(0, 0).start()

    loads[9].wait()

    def where_is(face):
        cell = cells[pl.ds(face, 1), :]
        cx = quotient(cell, total_z * ny)
        rest = cell - cx * (total_z * ny)
        cz = quotient(rest, ny)
        return cx - box * wx, cz - slab * wz, rest - cz * ny

    def hot(n, at):
        return jnp.where(iota((n, pts), 0) == at, 1.0, 0.0).astype(BF16)

    tall_x, tall_z = wx + 2 * MARGIN, wz + 2 * MARGIN
    px, pz, py = where_is(face_x)
    row_x[...] = hot(tall_z, jnp.where((px >= 0) & (px < wx), pz + MARGIN, -1))
    hot_x[...] = hot(ny, py)
    px, pz, py = where_is(jnp.where(slab == 0, 2, 3))
    row_z[...] = hot(tall_x, jnp.where((pz >= 0) & (pz < wz), px + MARGIN, -1))
    hot_z[...] = hot(ny, py)
    for face, row_hot, hot_at in ((4, row_low, hot_low), (5, row_high, hot_high)):
        px, pz, py = where_is(face)
        row_hot[...] = hot(tall_z, pz + MARGIN)
        hot_at[...] = hot(WIDE, px + MARGIN)


    for d in range(1, n_slab):
        give(d, 0).wait_recv()

    @pl.when(box_edge)
    def _():
        for d in range(1, n_slab):
            give(d, 1).wait_recv()

    @pl.when(slab_edge)
    def _():
        for d in range(1, n_slab):
            give(d, 2).wait_recv()

    values_y, values_x, values_z = ysend[...], xvsend[...], zvsend[jnp.where(slab == 0, 0, 1)]
    for d in range(1, n_slab):
        values_y = values_y + yrecv[d - 1]
        values_x = values_x + xvrecv[d - 1]
        values_z = values_z + zvrecv[d - 1]
    values_x = jnp.where(box_edge, values_x, 0.0)
    values_z = jnp.where(slab_edge, values_z, 0.0)

    def rows_of(v, k):
        return [v[k + t : k + t + 1] for t in both]

    low_y = place(row_low, rows_of(values_y, 0), hot_low)
    high_y = place(row_high, rows_of(values_y, steps), hot_high)
    on_z = place(row_z, rows_of(values_z, 0), hot_z)
    on_x = place(row_x, rows_of(values_x, 0), hot_x)
    for a in range(2):
        @pl.when(hears_box[a])
        def _(a=a):
            for c in x_copies(a, given):
                c.wait_recv()
    for a in range(2):
        plane = edge_x[1 - a]
        for m in range(members):
            rows = pl.ds((m * wx + plane) * wz, wz)
            ghost = jnp.where(hears_box[a], xghost[a, m], 0.0)
            one[rows, :] = psend[1 - a, m] + coef[rows, :] * ghost
    for b in range(2):
        @pl.when(hears_slab[b])
        def _(b=b):
            z_copy(b, 0).wait_recv()
            row = edge_z[1 - b]
            for m in range(members):
                for x in range(wx):
                    at = pl.ds((m * wx + x) * wz + row, 1)
                    one[at, :] += coef[at, :] * zghost[b, m, x : x + 1, :]

    for a in range(2):
        for b in range(2):
            @pl.when(hears_box[a] & hears_slab[b])
            def _(a=a, b=b):
                corner_copy(a, b).wait_recv()
    for b in range(2):
        @pl.when(hears_slab[b])
        def _(b=b):
            z_copy(b, 1).wait_recv()
    for a in range(2):
        @pl.when(hears_box[a])
        def _(a=a):
            x_copies(a, parts)[0].wait_recv()

    def across(a, b, m):
        return jnp.where(hears_box[a] & hears_slab[b], corner[a, b, m : m + 1, :], 0.0)

    for a in range(2):
        for m in range(members):
            beside = now[pl.ds((m * wx + edge_x[1 - a]) * wz, wz), :]
            beside = beside + jnp.where(z_at == 0, across(a, 0, m), 0.0)
            beside = beside + jnp.where(z_at == wz - 1, across(a, 1, m), 0.0)
            xout[a, m] = jnp.where(hears_box[a], xpart[a, m] + xcour[a] * gains[m] * beside, 0.0)
    for b in range(2):
        for m in range(members):
            beside = zsend[1 - b, m]
            beside = beside + jnp.where(x_at == 0, across(0, b, m), 0.0)
            beside = beside + jnp.where(x_at == wx - 1, across(1, b, m), 0.0)
            zout[b, m] = jnp.where(hears_slab[b], zpart[b, m] + zghost[b, members] * gains_beyond[m][b] * beside, 0.0)

    plane_x = jnp.where(box == 0, 0, wx - 1)
    line_z = jnp.where(slab == 0, 0, wz - 1)
    tiles = ny // 128

    def source(t, x, k, first, count):
        rows = slice(first + MARGIN, first + MARGIN + count)
        lanes = slice(k * 128, (k + 1) * 128)
        at = x + MARGIN
        lane = iota((count, 128), 1)
        out = jnp.where(iota((count, 128), 0) + first == line_z, on_z[t][at : at + 1, lanes], 0.0)
        if k == 0:
            out = out + jnp.where(lane == 0, low_y[t][rows, at : at + 1], 0.0)
        if k == tiles - 1:
            out = out + jnp.where(lane == 127, high_y[t][rows, at : at + 1], 0.0)
        if x in (0, wx - 1):
            out = out + jnp.where(plane_x == x, on_x[t][rows, lanes], 0.0)
        return out

    for k in range(tiles):
        lanes = slice(k * 128, (k + 1) * 128)
        for x in range(wx):
            plane = source(0, x, k, -MARGIN, tall_z)
            for b, row in ((0, MARGIN - 1), (1, MARGIN + wz)):
                line = plane[row : row + 1]
                for m in range(members):
                    zout[b, m, x : x + 1, lanes] += line
            for m in range(members):
                one[pl.ds((m * wx + x) * wz, wz), lanes] += plane[MARGIN : MARGIN + wz]
            src[pl.ds(x * wz, wz), lanes] = source(1, x, k, 0, wz)
        for a, x in ((0, -1), (1, wx)):
            plane = source(0, x, k, 0, wz)
            for m in range(members):
                xout[a, m, :, lanes] += plane

    for a in range(2):
        @pl.when(sends_box[a])
        def _(a=a):
            for c in x_copies(a, (*given, *parts)):
                c.wait_send()
            for b in range(2):
                @pl.when(sends_slab[b])
                def _(b=b):
                    corner_copy(a, b).wait_send()
    for b in range(2):
        @pl.when(sends_slab[b])
        def _(b=b):
            for i in range(2):
                z_copy(b, i).wait_send()
    for d in range(1, n_slab):
        give_all(d, lambda c: c.wait_send())


def last_kernel(dims, one, now, coef, xout, zout, src, next_h, last_h, two, sem):
    members, wx, wz, ny = dims[:4]
    group = 4 if wx % 4 == 0 else 1
    parts = wx // group
    last = pltpu.make_async_copy(one, last_h, sem.at[members * parts])
    last.start()
    z_at, y_at = iota((wz, ny), 0), iota((wz, ny), 1)

    def put(m, g):
        rows = pl.ds((m * wx + g * group) * wz, group * wz)
        return pltpu.make_async_copy(two.at[rows], next_h.at[rows], sem.at[m * parts + g])

    for m in range(members):
        for x in range(wx):
            at = (m * wx + x) * wz
            rows = pl.ds(at, wz)
            c = one[rows, :]
            lap = along_y(c, y_at) - 6.0 * c
            lap = lap + (one[pl.ds(at - wz, wz), :] if x > 0 else xout[0, m])
            lap = lap + (one[pl.ds(at + wz, wz), :] if x < wx - 1 else xout[1, m])
            lap = lap + jnp.where(z_at == 0, zout[0, m, x : x + 1, :], pltpu.roll(c, 1, 0))
            lap = lap + jnp.where(z_at == wz - 1, zout[1, m, x : x + 1, :], pltpu.roll(c, wz - 1, 0))
            two[rows, :] = (2.0 * c - now[rows, :]) + coef[rows, :] * lap + src[pl.ds(x * wz, wz), :]
            if x % group == group - 1:
                put(m, x // group).start()
    last.wait()
    for m in range(members):
        for g in range(parts):
            put(m, g).wait()


def on_device(pressure_now, pressure_prev, courant_sq, member_profiles, member_ids, stored_slabs,
              slab_home, interp_weights, surface_cells):
    members, wx, wz, ny = pressure_now.shape
    slots, length, points = stored_slabs.shape
    pts = surface_cells.shape[1]
    n_box, n_slab = lax.axis_size("box"), lax.axis_size("slab")
    dims = (members, wx, wz, ny, slots, length, pts, n_box, n_slab)
    rows = members * wx * wz
    peers = n_slab - 1
    tall_x, tall_z = wx + 2 * MARGIN, wz + 2 * MARGIN
    vmem = pl.BlockSpec(memory_space=pltpu.VMEM)
    in_hbm = lambda a: pltpu.with_memory_space_constraint(a, pltpu.HBM)
    hbm = pl.BlockSpec(memory_space=pltpu.HBM)
    struct = lambda *shape: jax.ShapeDtypeStruct(shape, F32)
    f32 = lambda *shape: pltpu.VMEM(shape, F32)
    bf16 = lambda *shape: pltpu.VMEM(shape, BF16)
    dma = pltpu.SemaphoreType.DMA
    kept = pl.pallas_call(
        functools.partial(kernel, dims),
        out_shape=(struct(rows, ny), struct(rows, ny), struct(rows, ny),
                   struct(2, members, wz, ny), struct(2, members, wx, ny), struct(wx * wz, ny)),
        in_specs=[pl.BlockSpec(memory_space=pltpu.SMEM)] + [hbm] * 8,
        out_specs=(vmem,) * 6,
        scratch_shapes=[
            pltpu.SMEM(member_ids.shape, I32),
            pltpu.VMEM(member_profiles.shape, F32), pltpu.VMEM(interp_weights.shape, F32),
            pltpu.VMEM(surface_cells.shape, I32),
            f32(rows, ny), f32(wx * wz, ny),
            f32(slots * length, 2 * pts), f32(slots * length, 2 * pts), f32(slots * length, pts),
            f32(2, members, wz, ny), f32(2, members + 1, wx, ny), f32(2, members, wx, ny), f32(2, 2, members, ny),
            f32(2, members, wz, ny), f32(2, wz, ny), f32(2, members, wz, ny),
            f32(2, members + 1, wx, ny), f32(2, members, wx, ny), f32(2, 2, members, ny),
            bf16(tall_z, pts), bf16(tall_x, pts), bf16(tall_z, pts), bf16(tall_z, pts),
            bf16(ny, pts), bf16(ny, pts), bf16(WIDE, pts), bf16(WIDE, pts),
            f32(4, pts), f32(2, pts), f32(2, 2, pts),
            f32(peers, 4, pts), f32(peers, 2, pts), f32(peers, 2, pts),
            dma((10,)), dma((4, members + 2)), dma((4, members + 2)), dma((2, 2)), dma((2, 2)),
            dma((peers, 3)), dma((peers, 3)), pltpu.SemaphoreType.REGULAR((2,)), pltpu.SemaphoreType.REGULAR((peers,)),
        ],
        compiler_params=pltpu.CompilerParams(collective_id=0, has_side_effects=True,
                                             vmem_limit_bytes=32 * 1024 * 1024),
    )(slab_home, *(in_hbm(a) for a in (
        member_ids, member_profiles, interp_weights, surface_cells,
        pressure_now.reshape(rows, ny), pressure_prev.reshape(rows, ny),
        courant_sq.reshape(wx * wz, ny), stored_slabs.reshape(slots * length, points),
    )))
    placed = pltpu.HBM((rows, ny), F32)
    new, last = pl.pallas_call(
        functools.partial(last_kernel, dims),
        out_shape=(placed, placed),
        in_specs=[vmem] * 6,
        out_specs=(hbm, hbm),
        scratch_shapes=[f32(rows, ny), dma((members * wx + 1,))],
        compiler_params=pltpu.CompilerParams(vmem_limit_bytes=4 * 1024 * 1024),
    )(*kept)
    return new.reshape(pressure_now.shape), last.reshape(pressure_now.shape)


def solution(mesh):
    in_specs = (
        P("ens", "box", "slab", None), P("ens", "box", "slab", None), P("box", "slab", None), P(),
        P("ens"), P("slab", None, None), P("ens"), P(), P(),
    )
    out_specs = (P("ens", "box", "slab", None), P("ens", "box", "slab", None))
    return jax.shard_map(on_device, mesh=mesh, in_specs=in_specs, out_specs=out_specs, check_vma=False)
```

```python
import functools

import jax
import jax.numpy as jnp
from jax import lax
from jax.experimental import pallas as pl
from jax.experimental.pallas import tpu as pltpu
from jax.sharding import PartitionSpec as P

F32, BF16, I32 = jnp.float32, jnp.bfloat16, jnp.int32
MESH = pl.DeviceIdType.MESH
MARGIN = 8


def iota(shape, dim):
    return lax.broadcasted_iota(I32, shape, dim)


def quotient(values, divisor):
    if divisor & (divisor - 1) == 0:
        return lax.shift_right_logical(values, divisor.bit_length() - 1)
    return lax.div(values, jnp.full_like(values, divisor))


def split2(v):
    high = v.astype(BF16).astype(F32)
    return high, v - high


def place(row_hot, values, right):
    rows = row_hot.shape[0]
    parts = []
    for v in values:
        for term in split2(v):
            wide = jnp.broadcast_to(term, (16, v.shape[1])).astype(BF16)
            parts += [row_hot[r : r + 16, :] * wide for r in range(0, rows, 16)]
    left = jnp.concatenate(parts, axis=0)
    sums = lax.dot_general(left, right[...], (((1,), (1,)), ((), ())), preferred_element_type=F32)
    return [sums[2 * t * rows : (2 * t + 1) * rows] + sums[(2 * t + 1) * rows : (2 * t + 2) * rows]
            for t in range(len(values))]


def along_y(c, y_at):
    ny = c.shape[1]
    return (jnp.where(y_at == 0, 0.0, pltpu.roll(c, 1, 1))
            + jnp.where(y_at == ny - 1, 0.0, pltpu.roll(c, ny - 1, 1)))


def kernel(dims, home, ids_h, prof_h, weights_h, cells_h, now_h, prev_h, cour_h, slabs_h,
           one, now, coef, xout, zout, src,
           ids, prof, weights, cells, prev, cour, slab_y, slab_z, slab_x,
           psend, zsend, zpsend, csend, xghost, xcour, xpart, zghost, zpart, corner,
           row_x, row_z, row_low, row_high, hot_x, hot_z, hot_low, hot_high,
           ysend, xvsend, zvsend, yrecv, xvrecv, zvrecv, xadd, zadd,
           load_sem, hs_sem, hr_sem, cs_sem, cr_sem, vs_sem, vr_sem, here_sem, peer_sem):
    members, wx, wz, ny, slots, length, pts, n_box, n_slab = dims
    steps = 2
    block = wx * wz
    box, slab = lax.axis_index("box"), lax.axis_index("slab")
    face_x = jnp.where(box == 0, 0, 1)
    box_edge = (box == 0) | (box == n_box - 1)
    slab_edge = (slab == 0) | (slab == n_slab - 1)
    pairs = (
        (slabs_h.at[:, pl.ds(4 * pts, 2 * pts)], slab_y), (weights_h, weights),
        (slabs_h.at[:, pl.ds(2 * pts, 2 * pts)], slab_z),
        (slabs_h.at[:, pl.ds(pl.multiple_of(face_x * pts, 128), pts)], slab_x),
        (now_h, now), (cour_h, cour), (prof_h, prof), (ids_h, ids), (prev_h, prev), (cells_h, cells))
    loads = [pltpu.make_async_copy(src_, dst, load_sem.at[i]) for i, (src_, dst) in enumerate(pairs)]

    barrier = pltpu.get_barrier_semaphore()

    def greet(target):
        pl.semaphore_signal(barrier, inc=1, device_id=target, device_id_type=MESH)

    sends_box = (box < n_box - 1, box > 0)
    sends_slab = (slab < n_slab - 1, slab > 0)
    hears_box = (box > 0, box < n_box - 1)
    hears_slab = (slab > 0, slab < n_slab - 1)
    shift = (1, -1)

    @pl.when(sends_box[0])
    def _():
        greet({"box": box + 1})

    @pl.when(sends_box[0] & sends_slab[0])
    def _():
        greet({"box": box + 1, "slab": slab + 1})

    for d in range(1, n_slab):
        @pl.when(slab + d < n_slab)
        def _(d=d):
            greet({"slab": slab + d})
    for c in loads:
        c.start()
    lower_box = jnp.where(box > 0, 1, 0)

    @pl.when((box > 0) | (slab > 0))
    def _():
        pl.semaphore_wait(barrier, slab + lower_box * jnp.where(slab > 0, 2, 1))

    def tell(ref, target):
        pl.semaphore_signal(ref, inc=1, device_id=target, device_id_type=MESH)

    @pl.when(sends_box[1])
    def _():
        tell(here_sem.at[0], {"box": box - 1})

    for d in range(1, n_slab):
        @pl.when(slab >= d)
        def _(d=d):
            tell(peer_sem.at[d - 1], {"slab": slab - d})

    @pl.when(sends_box[1] & sends_slab[1])
    def _():
        tell(here_sem.at[1], {"box": box - 1, "slab": slab - 1})

    for i in range(4):
        loads[i].wait()
    eye = iota((length, length), 0) == iota((length, length), 1)
    cols = []
    for t in range(steps):
        col = jnp.sum(jnp.where(eye, weights[t : t + 1, :], 0.0), axis=1, keepdims=True)
        cols.append([jnp.where(home[0] == slab * slots + s, col, 0.0) for s in range(slots)])

    def offered(ref, at, t):
        where = pl.ds(at, pts)
        total = cols[t][0] * ref[pl.ds(0, length), where]
        for s in range(1, slots):
            total = total + cols[t][s] * ref[pl.ds(s * length, length), where]
        return jnp.sum(total, axis=0, keepdims=True)

    both = range(steps)
    ysend[...] = jnp.concatenate([offered(slab_y, f * pts, t) for f in range(2) for t in both], axis=0)
    for f in range(2):
        zvsend[f] = jnp.concatenate([offered(slab_z, f * pts, t) for t in both], axis=0)
    xvsend[...] = jnp.concatenate([offered(slab_x, 0, t) for t in both], axis=0)

    def give(d, kind):
        peer = lax.rem(slab + d, n_slab)
        ref, into = ((ysend, yrecv), (xvsend, xvrecv), (zvsend.at[0], zvrecv), (zvsend.at[1], zvrecv))[kind]
        k = min(kind, 2)
        return pltpu.make_async_remote_copy(
            ref, into.at[d - 1], vs_sem.at[d - 1, k], vr_sem.at[d - 1, k],
            device_id={"slab": peer}, device_id_type=MESH)

    def gives(d, kind):
        peer = lax.rem(slab + d, n_slab)
        return (None, box_edge, peer == 0, peer == n_slab - 1)[kind]

    def give_all(d, act):
        for kind in range(4):
            cond = gives(d, kind)
            if cond is None:
                act(give(d, kind))
            else:
                @pl.when(cond)
                def _(kind=kind):
                    act(give(d, kind))

    for d in range(1, n_slab):
        @pl.when(slab + d >= n_slab)
        def _(d=d):
            give_all(d, lambda c: c.start())

    loads[4].wait()
    loads[5].wait()
    edge_x, edge_z = (wx - 1, 0), (wz - 1, 0)
    for b in range(2):
        for x in range(wx):
            for m in range(members):
                zsend[b, m, x : x + 1, :] = now[pl.ds((m * wx + x) * wz + edge_z[b], 1), :]
            zsend[b, members, x : x + 1, :] = cour[pl.ds(x * wz + edge_z[b], 1), :]
        for a in range(2):
            for m in range(members):
                csend[a, b, m : m + 1, :] = now[pl.ds((m * wx + edge_x[a]) * wz + edge_z[b], 1), :]

    given, parts = range(members + 1), range(members + 1, members + 2)

    def x_copies(a, which):
        peer = {"box": box + shift[a]}
        refs = [(now.at[pl.ds((m * wx + edge_x[a]) * wz, wz)], xghost.at[a, m]) for m in range(members)]
        refs += [(cour.at[pl.ds(edge_x[a] * wz, wz)], xcour.at[a]), (psend.at[a], xpart.at[a])]
        return [pltpu.make_async_remote_copy(*refs[i], hs_sem.at[a, i], hr_sem.at[a, i], device_id=peer, device_id_type=MESH)
                for i in which]

    def z_copy(b, i):
        source_, target = ((zsend.at[b], zghost.at[b]), (zpsend.at[b], zpart.at[b]))[i]
        return pltpu.make_async_remote_copy(source_, target, hs_sem.at[2 + b, i], hr_sem.at[2 + b, i],
                                            device_id={"slab": slab + shift[b]}, device_id_type=MESH)

    def corner_copy(a, b):
        return pltpu.make_async_remote_copy(
            csend.at[a, b], corner.at[a, b], cs_sem.at[a, b], cr_sem.at[a, b],
            device_id={"box": box + shift[a], "slab": slab + shift[b]}, device_id_type=MESH)

    @pl.when(sends_box[1])
    def _():
        for c in x_copies(1, given):
            c.start()

    @pl.when(sends_slab[1])
    def _():
        z_copy(1, 0).start()

    @pl.when(sends_box[1] & sends_slab[1])
    def _():
        corner_copy(1, 1).start()

    loads[6].wait()
    loads[7].wait()
    bank, total_z = prof.shape
    here = iota((wz, total_z), 1) == slab * wz + iota((wz, total_z), 0)
    beyond = [iota((1, total_z), 1) == slab * wz + at for at in (-1, wz)]
    gains, gains_beyond = [], []
    for m in range(members):
        mine = jnp.sum(jnp.where(iota((bank, total_z), 0) == ids[m], prof[...], 0.0), axis=0, keepdims=True)
        gains.append(1.0 + jnp.sum(jnp.where(here, mine, 0.0), axis=1, keepdims=True))
        gains_beyond.append([1.0 + jnp.sum(jnp.where(at, mine, 0.0), axis=1, keepdims=True) for at in beyond])

    loads[8].wait()
    z_at, y_at, x_at = iota((wz, ny), 0), iota((wz, ny), 1), iota((wx, ny), 0)
    for m in range(members):
        for x in (0, wx - 1, *range(1, wx - 1)):
            at = (m * wx + x) * wz
            rows = pl.ds(at, wz)
            c = now[rows, :]
            k = cour[pl.ds(x * wz, wz), :] * gains[m]
            coef[rows, :] = k
            lap = along_y(c, y_at) - 6.0 * c
            if x > 0:
                lap = lap + now[pl.ds(at - wz, wz), :]
            if x < wx - 1:
                lap = lap + now[pl.ds(at + wz, wz), :]
            lap = lap + jnp.where(z_at == 0, 0.0, pltpu.roll(c, 1, 0))
            lap = lap + jnp.where(z_at == wz - 1, 0.0, pltpu.roll(c, wz - 1, 0))
            nxt = (2.0 * c - prev[rows, :]) + k * lap
            if x == wx - 1:
                psend[0, m] = nxt
            elif x == 0:
                psend[1, m] = nxt
            else:
                one[rows, :] = nxt
            for b in range(2):
                zpsend[b, m, x : x + 1, :] = nxt[edge_z[b] : edge_z[b] + 1, :]
    @pl.when(sends_box[1])
    def _():
        x_copies(1, parts)[0].start()

    @pl.when(sends_slab[1])
    def _():
        z_copy(1, 1).start()

    for d in range(1, n_slab):
        @pl.when(slab + d < n_slab)
        def _(d=d):
            pl.semaphore_wait(peer_sem.at[d - 1], 1)
            give_all(d, lambda c: c.start())
            if d == 1:
                for i in range(2):
                    z_copy(0, i).start()

                @pl.when(sends_box[1])
                def _():
                    corner_copy(1, 0).start()

    @pl.when(sends_box[0])
    def _():
        pl.semaphore_wait(here_sem.at[0], 1)
        for c in x_copies(0, (*given, *parts)):
            c.start()

        @pl.when(sends_slab[1])
        def _():
            corner_copy(0, 1).start()

    @pl.when(sends_box[0] & sends_slab[0])
    def _():
        pl.semaphore_wait(here_sem.at[1], 1)
        corner_copy(0, 0).start()

    loads[9].wait()

    def where_is(face):
        cell = cells[pl.ds(face, 1), :]
        cx = quotient(cell, total_z * ny)
        rest = cell - cx * (total_z * ny)
        cz = quotient(rest, ny)
        return cx - box * wx, cz - slab * wz, rest - cz * ny

    def hot(n, at):
        return jnp.where(iota((n, pts), 0) == at, 1.0, 0.0).astype(BF16)

    tall_x, tall_z = wx + 2 * MARGIN, wz + 2 * MARGIN
    px, pz, py = where_is(face_x)
    row_x[...] = hot(tall_z, jnp.where((px >= 0) & (px < wx), pz + MARGIN, -1))
    hot_x[...] = hot(ny, py)
    px, pz, py = where_is(jnp.where(slab == 0, 2, 3))
    row_z[...] = hot(tall_x, jnp.where((pz >= 0) & (pz < wz), px + MARGIN, -1))
    hot_z[...] = hot(ny, py)
    for face, row_hot, hot_at in ((4, row_low, hot_low), (5, row_high, hot_high)):
        px, pz, py = where_is(face)
        row_hot[...] = hot(tall_z, pz + MARGIN)
        hot_at[...] = hot(tall_x, px + MARGIN)


    for a in range(2):
        @pl.when(sends_box[a])
        def _(a=a):
            for c in x_copies(a, (*given, *parts)):
                c.wait_send()
            for b in range(2):
                @pl.when(sends_slab[b])
                def _(b=b):
                    corner_copy(a, b).wait_send()
    for b in range(2):
        @pl.when(sends_slab[b])
        def _(b=b):
            for i in range(2):
                z_copy(b, i).wait_send()
    for d in range(1, n_slab):
        give_all(d, lambda c: c.wait_send())

    for d in range(1, n_slab):
        give(d, 0).wait_recv()

    @pl.when(box_edge)
    def _():
        for d in range(1, n_slab):
            give(d, 1).wait_recv()

    @pl.when(slab_edge)
    def _():
        for d in range(1, n_slab):
            give(d, 2).wait_recv()

    values_y, values_x, values_z = ysend[...], xvsend[...], zvsend[jnp.where(slab == 0, 0, 1)]
    for d in range(1, n_slab):
        values_y = values_y + yrecv[d - 1]
        values_x = values_x + xvrecv[d - 1]
        values_z = values_z + zvrecv[d - 1]
    values_x = jnp.where(box_edge, values_x, 0.0)
    values_z = jnp.where(slab_edge, values_z, 0.0)

    def rows_of(v, k):
        return [v[k + t : k + t + 1] for t in both]

    low_y = place(row_low, rows_of(values_y, 0), hot_low)
    high_y = place(row_high, rows_of(values_y, steps), hot_high)
    on_z = place(row_z, rows_of(values_z, 0), hot_z)
    on_x = place(row_x, rows_of(values_x, 0), hot_x)
    for a in range(2):
        @pl.when(hears_box[a])
        def _(a=a):
            for c in x_copies(a, given):
                c.wait_recv()
    for a in range(2):
        plane = edge_x[1 - a]
        for m in range(members):
            rows = pl.ds((m * wx + plane) * wz, wz)
            ghost = jnp.where(hears_box[a], xghost[a, m], 0.0)
            one[rows, :] = psend[1 - a, m] + coef[rows, :] * ghost
    for b in range(2):
        @pl.when(hears_slab[b])
        def _(b=b):
            z_copy(b, 0).wait_recv()
            row = edge_z[1 - b]
            for m in range(members):
                for x in range(wx):
                    at = pl.ds((m * wx + x) * wz + row, 1)
                    one[at, :] += coef[at, :] * zghost[b, m, x : x + 1, :]

    plane_x = jnp.where(box == 0, 0, wx - 1)
    line_z = jnp.where(slab == 0, 0, wz - 1)
    tiles = ny // 128

    def source(t, x, k, first, count):
        rows = slice(first + MARGIN, first + MARGIN + count)
        lanes = slice(k * 128, (k + 1) * 128)
        at = x + MARGIN
        lane = iota((count, 128), 1)
        out = jnp.where(iota((count, 128), 0) + first == line_z, on_z[t][at : at + 1, lanes], 0.0)
        if k == 0:
            out = out + jnp.where(lane == 0, low_y[t][rows, at : at + 1], 0.0)
        if k == tiles - 1:
            out = out + jnp.where(lane == 127, high_y[t][rows, at : at + 1], 0.0)
        if x in (0, wx - 1):
            out = out + jnp.where(plane_x == x, on_x[t][rows, lanes], 0.0)
        return out

    for k in range(tiles):
        lanes = slice(k * 128, (k + 1) * 128)
        for x in range(wx):
            plane = source(0, x, k, -MARGIN, tall_z)
            for b, row in ((0, MARGIN - 1), (1, MARGIN + wz)):
                line = plane[row : row + 1]
                zadd[b, x : x + 1, lanes] = line
            for m in range(members):
                one[pl.ds((m * wx + x) * wz, wz), lanes] += plane[MARGIN : MARGIN + wz]
            src[pl.ds(x * wz, wz), lanes] = source(1, x, k, 0, wz)
        for a, x in ((0, -1), (1, wx)):
            xadd[a, :, lanes] = source(0, x, k, 0, wz)

    for a in range(2):
        for b in range(2):
            @pl.when(hears_box[a] & hears_slab[b])
            def _(a=a, b=b):
                corner_copy(a, b).wait_recv()
    for b in range(2):
        @pl.when(hears_slab[b])
        def _(b=b):
            z_copy(b, 1).wait_recv()
    for a in range(2):
        @pl.when(hears_box[a])
        def _(a=a):
            x_copies(a, parts)[0].wait_recv()

    def across(a, b, m):
        return jnp.where(hears_box[a] & hears_slab[b], corner[a, b, m : m + 1, :], 0.0)

    for a in range(2):
        for m in range(members):
            beside = now[pl.ds((m * wx + edge_x[1 - a]) * wz, wz), :]
            beside = beside + jnp.where(z_at == 0, across(a, 0, m), 0.0)
            beside = beside + jnp.where(z_at == wz - 1, across(a, 1, m), 0.0)
            xout[a, m] = jnp.where(hears_box[a], (xpart[a, m] + xadd[a]) + xcour[a] * gains[m] * beside, 0.0)
    for b in range(2):
        for m in range(members):
            beside = zsend[1 - b, m]
            beside = beside + jnp.where(x_at == 0, across(0, b, m), 0.0)
            beside = beside + jnp.where(x_at == wx - 1, across(1, b, m), 0.0)
            zout[b, m] = jnp.where(hears_slab[b], (zpart[b, m] + zadd[b]) + zghost[b, members] * gains_beyond[m][b] * beside, 0.0)


def last_kernel(dims, one, now, coef, xout, zout, src, next_h, last_h, two, sem):
    members, wx, wz, ny = dims[:4]
    group = 4 if wx % 4 == 0 else 1
    parts = wx // group
    last = pltpu.make_async_copy(one, last_h, sem.at[members * parts])
    last.start()
    z_at, y_at = iota((wz, ny), 0), iota((wz, ny), 1)

    def put(m, g):
        rows = pl.ds((m * wx + g * group) * wz, group * wz)
        return pltpu.make_async_copy(two.at[rows], next_h.at[rows], sem.at[m * parts + g])

    for m in range(members):
        for x in range(wx):
            at = (m * wx + x) * wz
            rows = pl.ds(at, wz)
            c = one[rows, :]
            lap = along_y(c, y_at) - 6.0 * c
            lap = lap + (one[pl.ds(at - wz, wz), :] if x > 0 else xout[0, m])
            lap = lap + (one[pl.ds(at + wz, wz), :] if x < wx - 1 else xout[1, m])
            lap = lap + jnp.where(z_at == 0, zout[0, m, x : x + 1, :], pltpu.roll(c, 1, 0))
            lap = lap + jnp.where(z_at == wz - 1, zout[1, m, x : x + 1, :], pltpu.roll(c, wz - 1, 0))
            two[rows, :] = (2.0 * c - now[rows, :]) + coef[rows, :] * lap + src[pl.ds(x * wz, wz), :]
            if x % group == group - 1:
                put(m, x // group).start()
    last.wait()
    for m in range(members):
        for g in range(parts):
            put(m, g).wait()


def on_device(pressure_now, pressure_prev, courant_sq, member_profiles, member_ids, stored_slabs,
              slab_home, interp_weights, surface_cells):
    members, wx, wz, ny = pressure_now.shape
    slots, length, points = stored_slabs.shape
    pts = surface_cells.shape[1]
    n_box, n_slab = lax.axis_size("box"), lax.axis_size("slab")
    dims = (members, wx, wz, ny, slots, length, pts, n_box, n_slab)
    rows = members * wx * wz
    peers = n_slab - 1
    tall_x, tall_z = wx + 2 * MARGIN, wz + 2 * MARGIN
    vmem = pl.BlockSpec(memory_space=pltpu.VMEM)
    in_hbm = lambda a: pltpu.with_memory_space_constraint(a, pltpu.HBM)
    hbm = pl.BlockSpec(memory_space=pltpu.HBM)
    struct = lambda *shape: jax.ShapeDtypeStruct(shape, F32)
    f32 = lambda *shape: pltpu.VMEM(shape, F32)
    bf16 = lambda *shape: pltpu.VMEM(shape, BF16)
    dma = pltpu.SemaphoreType.DMA
    kept = pl.pallas_call(
        functools.partial(kernel, dims),
        out_shape=(struct(rows, ny), struct(rows, ny), struct(rows, ny),
                   struct(2, members, wz, ny), struct(2, members, wx, ny), struct(wx * wz, ny)),
        in_specs=[pl.BlockSpec(memory_space=pltpu.SMEM)] + [hbm] * 8,
        out_specs=(vmem,) * 6,
        scratch_shapes=[
            pltpu.SMEM(member_ids.shape, I32),
            pltpu.VMEM(member_profiles.shape, F32), pltpu.VMEM(interp_weights.shape, F32),
            pltpu.VMEM(surface_cells.shape, I32),
            f32(rows, ny), f32(wx * wz, ny),
            f32(slots * length, 2 * pts), f32(slots * length, 2 * pts), f32(slots * length, pts),
            f32(2, members, wz, ny), f32(2, members + 1, wx, ny), f32(2, members, wx, ny), f32(2, 2, members, ny),
            f32(2, members, wz, ny), f32(2, wz, ny), f32(2, members, wz, ny),
            f32(2, members + 1, wx, ny), f32(2, members, wx, ny), f32(2, 2, members, ny),
            bf16(tall_z, pts), bf16(tall_x, pts), bf16(tall_z, pts), bf16(tall_z, pts),
            bf16(ny, pts), bf16(ny, pts), bf16(tall_x, pts), bf16(tall_x, pts),
            f32(4, pts), f32(2, pts), f32(2, 2, pts),
            f32(peers, 4, pts), f32(peers, 2, pts), f32(peers, 2, pts),
            f32(2, wz, ny), f32(2, wx, ny),
            dma((10,)), dma((4, members + 2)), dma((4, members + 2)), dma((2, 2)), dma((2, 2)),
            dma((peers, 3)), dma((peers, 3)), pltpu.SemaphoreType.REGULAR((2,)), pltpu.SemaphoreType.REGULAR((peers,)),
        ],
        compiler_params=pltpu.CompilerParams(collective_id=0, has_side_effects=True,
                                             vmem_limit_bytes=32 * 1024 * 1024),
    )(slab_home, *(in_hbm(a) for a in (
        member_ids, member_profiles, interp_weights, surface_cells,
        pressure_now.reshape(rows, ny), pressure_prev.reshape(rows, ny),
        courant_sq.reshape(wx * wz, ny), stored_slabs.reshape(slots * length, points),
    )))
    placed = pltpu.HBM((rows, ny), F32)
    new, last = pl.pallas_call(
        functools.partial(last_kernel, dims),
        out_shape=(placed, placed),
        in_specs=[vmem] * 6,
        out_specs=(hbm, hbm),
        scratch_shapes=[f32(rows, ny), dma((members * wx + 1,))],
        compiler_params=pltpu.CompilerParams(vmem_limit_bytes=4 * 1024 * 1024),
    )(*kept)
    return new.reshape(pressure_now.shape), last.reshape(pressure_now.shape)


def solution(mesh):
    in_specs = (
        P("ens", "box", "slab", None), P("ens", "box", "slab", None), P("box", "slab", None), P(),
        P("ens"), P("slab", None, None), P("ens"), P(), P(),
    )
    out_specs = (P("ens", "box", "slab", None), P("ens", "box", "slab", None))
    return jax.shard_map(on_device, mesh=mesh, in_specs=in_specs, out_specs=out_specs, check_vma=False)
```

```python
import functools

import jax
import jax.numpy as jnp
from jax import lax
from jax.experimental import pallas as pl
from jax.experimental.pallas import tpu as pltpu
from jax.sharding import PartitionSpec as P

F32, BF16, I32 = jnp.float32, jnp.bfloat16, jnp.int32
MESH = pl.DeviceIdType.MESH
MARGIN = 8


def iota(shape, dim):
    return lax.broadcasted_iota(I32, shape, dim)


def quotient(values, divisor):
    if divisor & (divisor - 1) == 0:
        return lax.shift_right_logical(values, divisor.bit_length() - 1)
    return lax.div(values, jnp.full_like(values, divisor))


def split2(v):
    high = v.astype(BF16).astype(F32)
    return high, v - high


def place(row_hot, values, right):
    rows = row_hot.shape[0]
    parts = []
    for v in values:
        for term in split2(v):
            wide = jnp.broadcast_to(term, (16, v.shape[1])).astype(BF16)
            parts += [row_hot[r : r + 16, :] * wide for r in range(0, rows, 16)]
    left = jnp.concatenate(parts, axis=0)
    sums = lax.dot_general(left, right[...], (((1,), (1,)), ((), ())), preferred_element_type=F32)
    return [sums[2 * t * rows : (2 * t + 1) * rows] + sums[(2 * t + 1) * rows : (2 * t + 2) * rows]
            for t in range(len(values))]


def along_y(c, y_at):
    ny = c.shape[1]
    return (jnp.where(y_at == 0, 0.0, pltpu.roll(c, 1, 1))
            + jnp.where(y_at == ny - 1, 0.0, pltpu.roll(c, ny - 1, 1)))


def kernel(dims, home, ids_h, prof_h, weights_h, cells_h, now_h, prev_h, cour_h, slabs_h,
           one, now, coef, xout, zout, src,
           ids, prof, weights, cells, prev, cour, slab_y, slab_z, slab_x,
           psend, zsend, zpsend, csend, xghost, xcour, xpart, zghost, zpart, corner,
           row_x, row_z, row_low, row_high, hot_x, hot_z, hot_low, hot_high,
           ysend, xvsend, zvsend, yrecv, xvrecv, zvrecv, xadd, zadd,
           load_sem, hs_sem, hr_sem, cs_sem, cr_sem, vs_sem, vr_sem, here_sem, peer_sem):
    members, wx, wz, ny, slots, length, pts, n_box, n_slab = dims
    steps = 2
    block = wx * wz
    box, slab = lax.axis_index("box"), lax.axis_index("slab")
    face_x = jnp.where(box == 0, 0, 1)
    box_edge = (box == 0) | (box == n_box - 1)
    slab_edge = (slab == 0) | (slab == n_slab - 1)
    pairs = (
        (slabs_h.at[:, pl.ds(4 * pts, 2 * pts)], slab_y), (weights_h, weights),
        (slabs_h.at[:, pl.ds(2 * pts, 2 * pts)], slab_z),
        (slabs_h.at[:, pl.ds(pl.multiple_of(face_x * pts, 128), pts)], slab_x),
        (now_h, now), (cour_h, cour), (prof_h, prof), (ids_h, ids), (prev_h, prev), (cells_h, cells))
    loads = [pltpu.make_async_copy(src_, dst, load_sem.at[i]) for i, (src_, dst) in enumerate(pairs)]

    barrier = pltpu.get_barrier_semaphore()

    def greet(target):
        pl.semaphore_signal(barrier, inc=1, device_id=target, device_id_type=MESH)

    sends_box = (box < n_box - 1, box > 0)
    sends_slab = (slab < n_slab - 1, slab > 0)
    hears_box = (box > 0, box < n_box - 1)
    hears_slab = (slab > 0, slab < n_slab - 1)
    shift = (1, -1)

    @pl.when(sends_box[0])
    def _():
        greet({"box": box + 1})

    @pl.when(sends_box[0] & sends_slab[0])
    def _():
        greet({"box": box + 1, "slab": slab + 1})

    for d in range(1, n_slab):
        @pl.when(slab + d < n_slab)
        def _(d=d):
            greet({"slab": slab + d})
    for c in loads:
        c.start()
    lower_box = jnp.where(box > 0, 1, 0)

    @pl.when((box > 0) | (slab > 0))
    def _():
        pl.semaphore_wait(barrier, slab + lower_box * jnp.where(slab > 0, 2, 1))

    def tell(ref, target):
        pl.semaphore_signal(ref, inc=1, device_id=target, device_id_type=MESH)

    @pl.when(sends_box[1])
    def _():
        tell(here_sem.at[0], {"box": box - 1})

    for d in range(1, n_slab):
        @pl.when(slab >= d)
        def _(d=d):
            tell(peer_sem.at[d - 1], {"slab": slab - d})

    @pl.when(sends_box[1] & sends_slab[1])
    def _():
        tell(here_sem.at[1], {"box": box - 1, "slab": slab - 1})

    for i in range(4):
        loads[i].wait()
    eye = iota((length, length), 0) == iota((length, length), 1)
    cols = []
    for t in range(steps):
        col = jnp.sum(jnp.where(eye, weights[t : t + 1, :], 0.0), axis=1, keepdims=True)
        cols.append([jnp.where(home[0] == slab * slots + s, col, 0.0) for s in range(slots)])

    def offered(ref, at, t):
        where = pl.ds(at, pts)
        total = cols[t][0] * ref[pl.ds(0, length), where]
        for s in range(1, slots):
            total = total + cols[t][s] * ref[pl.ds(s * length, length), where]
        return jnp.sum(total, axis=0, keepdims=True)

    both = range(steps)
    ysend[...] = jnp.concatenate([offered(slab_y, f * pts, t) for f in range(2) for t in both], axis=0)
    for f in range(2):
        zvsend[f] = jnp.concatenate([offered(slab_z, f * pts, t) for t in both], axis=0)
    xvsend[...] = jnp.concatenate([offered(slab_x, 0, t) for t in both], axis=0)

    def give(d, kind):
        peer = lax.rem(slab + d, n_slab)
        ref, into = ((ysend, yrecv), (xvsend, xvrecv), (zvsend.at[0], zvrecv), (zvsend.at[1], zvrecv))[kind]
        k = min(kind, 2)
        return pltpu.make_async_remote_copy(
            ref, into.at[d - 1], vs_sem.at[d - 1, k], vr_sem.at[d - 1, k],
            device_id={"slab": peer}, device_id_type=MESH)

    def gives(d, kind):
        peer = lax.rem(slab + d, n_slab)
        return (None, box_edge, peer == 0, peer == n_slab - 1)[kind]

    def give_all(d, act, kinds=range(4)):
        for kind in kinds:
            cond = gives(d, kind)
            if cond is None:
                act(give(d, kind))
            else:
                @pl.when(cond)
                def _(kind=kind):
                    act(give(d, kind))

    for kinds in ((0,), (1, 2, 3)):
        for d in range(1, n_slab):
            @pl.when(slab + d >= n_slab)
            def _(d=d, kinds=kinds):
                give_all(d, lambda c: c.start(), kinds)

    loads[4].wait()
    loads[5].wait()
    edge_x, edge_z = (wx - 1, 0), (wz - 1, 0)
    for b in range(2):
        for x in range(wx):
            for m in range(members):
                zsend[b, m, x : x + 1, :] = now[pl.ds((m * wx + x) * wz + edge_z[b], 1), :]
            zsend[b, members, x : x + 1, :] = cour[pl.ds(x * wz + edge_z[b], 1), :]
        for a in range(2):
            for m in range(members):
                csend[a, b, m : m + 1, :] = now[pl.ds((m * wx + edge_x[a]) * wz + edge_z[b], 1), :]

    given, parts = range(members + 1), range(members + 1, members + 2)

    def x_copies(a, which):
        peer = {"box": box + shift[a]}
        refs = [(now.at[pl.ds((m * wx + edge_x[a]) * wz, wz)], xghost.at[a, m]) for m in range(members)]
        refs += [(cour.at[pl.ds(edge_x[a] * wz, wz)], xcour.at[a]), (psend.at[a], xpart.at[a])]
        return [pltpu.make_async_remote_copy(*refs[i], hs_sem.at[a, i], hr_sem.at[a, i], device_id=peer, device_id_type=MESH)
                for i in which]

    def z_copy(b, i):
        source_, target = ((zsend.at[b], zghost.at[b]), (zpsend.at[b], zpart.at[b]))[i]
        return pltpu.make_async_remote_copy(source_, target, hs_sem.at[2 + b, i], hr_sem.at[2 + b, i],
                                            device_id={"slab": slab + shift[b]}, device_id_type=MESH)

    def corner_copy(a, b):
        return pltpu.make_async_remote_copy(
            csend.at[a, b], corner.at[a, b], cs_sem.at[a, b], cr_sem.at[a, b],
            device_id={"box": box + shift[a], "slab": slab + shift[b]}, device_id_type=MESH)

    @pl.when(sends_box[1])
    def _():
        for c in x_copies(1, given):
            c.start()

    @pl.when(sends_slab[1])
    def _():
        z_copy(1, 0).start()

    @pl.when(sends_box[1] & sends_slab[1])
    def _():
        corner_copy(1, 1).start()

    loads[6].wait()
    loads[7].wait()
    bank, total_z = prof.shape
    here = iota((wz, total_z), 1) == slab * wz + iota((wz, total_z), 0)
    beyond = [iota((1, total_z), 1) == slab * wz + at for at in (-1, wz)]
    gains, gains_beyond = [], []
    for m in range(members):
        mine = jnp.sum(jnp.where(iota((bank, total_z), 0) == ids[m], prof[...], 0.0), axis=0, keepdims=True)
        gains.append(1.0 + jnp.sum(jnp.where(here, mine, 0.0), axis=1, keepdims=True))
        gains_beyond.append([1.0 + jnp.sum(jnp.where(at, mine, 0.0), axis=1, keepdims=True) for at in beyond])

    loads[8].wait()
    z_at, y_at, x_at = iota((wz, ny), 0), iota((wz, ny), 1), iota((wx, ny), 0)
    for m in range(members):
        for x in (0, wx - 1, *range(1, wx - 1)):
            at = (m * wx + x) * wz
            rows = pl.ds(at, wz)
            c = now[rows, :]
            k = cour[pl.ds(x * wz, wz), :] * gains[m]
            coef[rows, :] = k
            lap = along_y(c, y_at) - 6.0 * c
            if x > 0:
                lap = lap + now[pl.ds(at - wz, wz), :]
            if x < wx - 1:
                lap = lap + now[pl.ds(at + wz, wz), :]
            lap = lap + jnp.where(z_at == 0, 0.0, pltpu.roll(c, 1, 0))
            lap = lap + jnp.where(z_at == wz - 1, 0.0, pltpu.roll(c, wz - 1, 0))
            nxt = (2.0 * c - prev[rows, :]) + k * lap
            if x == wx - 1:
                psend[0, m] = nxt
            elif x == 0:
                psend[1, m] = nxt
            else:
                one[rows, :] = nxt
            for b in range(2):
                zpsend[b, m, x : x + 1, :] = nxt[edge_z[b] : edge_z[b] + 1, :]
    @pl.when(sends_box[1])
    def _():
        x_copies(1, parts)[0].start()

    @pl.when(sends_slab[1])
    def _():
        z_copy(1, 1).start()

    for d in range(1, n_slab):
        @pl.when(slab + d < n_slab)
        def _(d=d):
            pl.semaphore_wait(peer_sem.at[d - 1], 1)
            give_all(d, lambda c: c.start())
            if d == 1:
                for i in range(2):
                    z_copy(0, i).start()

                @pl.when(sends_box[1])
                def _():
                    corner_copy(1, 0).start()

    @pl.when(sends_box[0])
    def _():
        pl.semaphore_wait(here_sem.at[0], 1)
        for c in x_copies(0, (*given, *parts)):
            c.start()

        @pl.when(sends_slab[1])
        def _():
            corner_copy(0, 1).start()

    @pl.when(sends_box[0] & sends_slab[0])
    def _():
        pl.semaphore_wait(here_sem.at[1], 1)
        corner_copy(0, 0).start()

    loads[9].wait()

    def where_is(face):
        cell = cells[pl.ds(face, 1), :]
        cx = quotient(cell, total_z * ny)
        rest = cell - cx * (total_z * ny)
        cz = quotient(rest, ny)
        return cx - box * wx, cz - slab * wz, rest - cz * ny

    def hot(n, at):
        return jnp.where(iota((n, pts), 0) == at, 1.0, 0.0).astype(BF16)

    tall_x, tall_z = wx + 2 * MARGIN, wz + 2 * MARGIN
    px, pz, py = where_is(face_x)
    row_x[...] = hot(tall_z, jnp.where((px >= 0) & (px < wx), pz + MARGIN, -1))
    hot_x[...] = hot(ny, py)
    px, pz, py = where_is(jnp.where(slab == 0, 2, 3))
    row_z[...] = hot(tall_x, jnp.where((pz >= 0) & (pz < wz), px + MARGIN, -1))
    hot_z[...] = hot(ny, py)
    for face, row_hot, hot_at in ((4, row_low, hot_low), (5, row_high, hot_high)):
        px, pz, py = where_is(face)
        row_hot[...] = hot(tall_z, pz + MARGIN)
        hot_at[...] = hot(tall_x, px + MARGIN)


    for a in range(2):
        @pl.when(sends_box[a])
        def _(a=a):
            for c in x_copies(a, (*given, *parts)):
                c.wait_send()
            for b in range(2):
                @pl.when(sends_slab[b])
                def _(b=b):
                    corner_copy(a, b).wait_send()
    for b in range(2):
        @pl.when(sends_slab[b])
        def _(b=b):
            for i in range(2):
                z_copy(b, i).wait_send()
    for d in range(1, n_slab):
        give_all(d, lambda c: c.wait_send())

    for d in range(1, n_slab):
        give(d, 0).wait_recv()

    values_y = ysend[...]
    for d in range(1, n_slab):
        values_y = values_y + yrecv[d - 1]

    def rows_of(v, k):
        return [v[k + t : k + t + 1] for t in both]

    low_y = place(row_low, rows_of(values_y, 0), hot_low)
    high_y = place(row_high, rows_of(values_y, steps), hot_high)

    @pl.when(box_edge)
    def _():
        for d in range(1, n_slab):
            give(d, 1).wait_recv()

    @pl.when(slab_edge)
    def _():
        for d in range(1, n_slab):
            give(d, 2).wait_recv()

    values_x, values_z = xvsend[...], zvsend[jnp.where(slab == 0, 0, 1)]
    for d in range(1, n_slab):
        values_x = values_x + xvrecv[d - 1]
        values_z = values_z + zvrecv[d - 1]
    values_x = jnp.where(box_edge, values_x, 0.0)
    values_z = jnp.where(slab_edge, values_z, 0.0)

    on_z = place(row_z, rows_of(values_z, 0), hot_z)
    on_x = place(row_x, rows_of(values_x, 0), hot_x)
    for a in range(2):
        @pl.when(hears_box[a])
        def _(a=a):
            for c in x_copies(a, given):
                c.wait_recv()
    for a in range(2):
        plane = edge_x[1 - a]
        for m in range(members):
            rows = pl.ds((m * wx + plane) * wz, wz)
            ghost = jnp.where(hears_box[a], xghost[a, m], 0.0)
            one[rows, :] = psend[1 - a, m] + coef[rows, :] * ghost
    for b in range(2):
        @pl.when(hears_slab[b])
        def _(b=b):
            z_copy(b, 0).wait_recv()
            row = edge_z[1 - b]
            for m in range(members):
                for x in range(wx):
                    at = pl.ds((m * wx + x) * wz + row, 1)
                    one[at, :] += coef[at, :] * zghost[b, m, x : x + 1, :]

    plane_x = jnp.where(box == 0, 0, wx - 1)
    line_z = jnp.where(slab == 0, 0, wz - 1)
    tiles = ny // 128

    def source(t, x, k, first, count):
        rows = slice(first + MARGIN, first + MARGIN + count)
        lanes = slice(k * 128, (k + 1) * 128)
        at = x + MARGIN
        lane = iota((count, 128), 1)
        out = jnp.where(iota((count, 128), 0) + first == line_z, on_z[t][at : at + 1, lanes], 0.0)
        if k == 0:
            out = out + jnp.where(lane == 0, low_y[t][rows, at : at + 1], 0.0)
        if k == tiles - 1:
            out = out + jnp.where(lane == 127, high_y[t][rows, at : at + 1], 0.0)
        if x in (0, wx - 1):
            out = out + jnp.where(plane_x == x, on_x[t][rows, lanes], 0.0)
        return out

    for k in range(tiles):
        lanes = slice(k * 128, (k + 1) * 128)
        for x in range(wx):
            plane = source(0, x, k, -MARGIN, tall_z)
            for b, row in ((0, MARGIN - 1), (1, MARGIN + wz)):
                line = plane[row : row + 1]
                zadd[b, x : x + 1, lanes] = line
            for m in range(members):
                one[pl.ds((m * wx + x) * wz, wz), lanes] += plane[MARGIN : MARGIN + wz]
            src[pl.ds(x * wz, wz), lanes] = source(1, x, k, 0, wz)
        for a, x in ((0, -1), (1, wx)):
            xadd[a, :, lanes] = source(0, x, k, 0, wz)

    for a in range(2):
        for b in range(2):
            @pl.when(hears_box[a] & hears_slab[b])
            def _(a=a, b=b):
                corner_copy(a, b).wait_recv()
    for b in range(2):
        @pl.when(hears_slab[b])
        def _(b=b):
            z_copy(b, 1).wait_recv()
    for a in range(2):
        @pl.when(hears_box[a])
        def _(a=a):
            x_copies(a, parts)[0].wait_recv()

    def across(a, b, m):
        return jnp.where(hears_box[a] & hears_slab[b], corner[a, b, m : m + 1, :], 0.0)

    for a in range(2):
        for m in range(members):
            beside = now[pl.ds((m * wx + edge_x[1 - a]) * wz, wz), :]
            beside = beside + jnp.where(z_at == 0, across(a, 0, m), 0.0)
            beside = beside + jnp.where(z_at == wz - 1, across(a, 1, m), 0.0)
            xout[a, m] = jnp.where(hears_box[a], (xpart[a, m] + xadd[a]) + xcour[a] * gains[m] * beside, 0.0)
    for b in range(2):
        for m in range(members):
            beside = zsend[1 - b, m]
            beside = beside + jnp.where(x_at == 0, across(0, b, m), 0.0)
            beside = beside + jnp.where(x_at == wx - 1, across(1, b, m), 0.0)
            zout[b, m] = jnp.where(hears_slab[b], (zpart[b, m] + zadd[b]) + zghost[b, members] * gains_beyond[m][b] * beside, 0.0)


def last_kernel(dims, one, now, coef, xout, zout, src, next_h, last_h, two, sem):
    members, wx, wz, ny = dims[:4]
    group = 4 if wx % 4 == 0 else 1
    parts = wx // group
    last = pltpu.make_async_copy(one, last_h, sem.at[members * parts])
    last.start()
    z_at, y_at = iota((wz, ny), 0), iota((wz, ny), 1)

    def put(m, g):
        rows = pl.ds((m * wx + g * group) * wz, group * wz)
        return pltpu.make_async_copy(two.at[rows], next_h.at[rows], sem.at[m * parts + g])

    for m in range(members):
        for x in range(wx):
            at = (m * wx + x) * wz
            rows = pl.ds(at, wz)
            c = one[rows, :]
            lap = along_y(c, y_at) - 6.0 * c
            lap = lap + (one[pl.ds(at - wz, wz), :] if x > 0 else xout[0, m])
            lap = lap + (one[pl.ds(at + wz, wz), :] if x < wx - 1 else xout[1, m])
            lap = lap + jnp.where(z_at == 0, zout[0, m, x : x + 1, :], pltpu.roll(c, 1, 0))
            lap = lap + jnp.where(z_at == wz - 1, zout[1, m, x : x + 1, :], pltpu.roll(c, wz - 1, 0))
            two[rows, :] = (2.0 * c - now[rows, :]) + coef[rows, :] * lap + src[pl.ds(x * wz, wz), :]
            if x % group == group - 1:
                put(m, x // group).start()
    last.wait()
    for m in range(members):
        for g in range(parts):
            put(m, g).wait()


def on_device(pressure_now, pressure_prev, courant_sq, member_profiles, member_ids, stored_slabs,
              slab_home, interp_weights, surface_cells):
    members, wx, wz, ny = pressure_now.shape
    slots, length, points = stored_slabs.shape
    pts = surface_cells.shape[1]
    n_box, n_slab = lax.axis_size("box"), lax.axis_size("slab")
    dims = (members, wx, wz, ny, slots, length, pts, n_box, n_slab)
    rows = members * wx * wz
    peers = n_slab - 1
    tall_x, tall_z = wx + 2 * MARGIN, wz + 2 * MARGIN
    vmem = pl.BlockSpec(memory_space=pltpu.VMEM)
    in_hbm = lambda a: pltpu.with_memory_space_constraint(a, pltpu.HBM)
    hbm = pl.BlockSpec(memory_space=pltpu.HBM)
    struct = lambda *shape: jax.ShapeDtypeStruct(shape, F32)
    f32 = lambda *shape: pltpu.VMEM(shape, F32)
    bf16 = lambda *shape: pltpu.VMEM(shape, BF16)
    dma = pltpu.SemaphoreType.DMA
    kept = pl.pallas_call(
        functools.partial(kernel, dims),
        out_shape=(struct(rows, ny), struct(rows, ny), struct(rows, ny),
                   struct(2, members, wz, ny), struct(2, members, wx, ny), struct(wx * wz, ny)),
        in_specs=[pl.BlockSpec(memory_space=pltpu.SMEM)] + [hbm] * 8,
        out_specs=(vmem,) * 6,
        scratch_shapes=[
            pltpu.SMEM(member_ids.shape, I32),
            pltpu.VMEM(member_profiles.shape, F32), pltpu.VMEM(interp_weights.shape, F32),
            pltpu.VMEM(surface_cells.shape, I32),
            f32(rows, ny), f32(wx * wz, ny),
            f32(slots * length, 2 * pts), f32(slots * length, 2 * pts), f32(slots * length, pts),
            f32(2, members, wz, ny), f32(2, members + 1, wx, ny), f32(2, members, wx, ny), f32(2, 2, members, ny),
            f32(2, members, wz, ny), f32(2, wz, ny), f32(2, members, wz, ny),
            f32(2, members + 1, wx, ny), f32(2, members, wx, ny), f32(2, 2, members, ny),
            bf16(tall_z, pts), bf16(tall_x, pts), bf16(tall_z, pts), bf16(tall_z, pts),
            bf16(ny, pts), bf16(ny, pts), bf16(tall_x, pts), bf16(tall_x, pts),
            f32(4, pts), f32(2, pts), f32(2, 2, pts),
            f32(peers, 4, pts), f32(peers, 2, pts), f32(peers, 2, pts),
            f32(2, wz, ny), f32(2, wx, ny),
            dma((10,)), dma((4, members + 2)), dma((4, members + 2)), dma((2, 2)), dma((2, 2)),
            dma((peers, 3)), dma((peers, 3)), pltpu.SemaphoreType.REGULAR((2,)), pltpu.SemaphoreType.REGULAR((peers,)),
        ],
        compiler_params=pltpu.CompilerParams(collective_id=0, has_side_effects=True,
                                             vmem_limit_bytes=32 * 1024 * 1024),
    )(slab_home, *(in_hbm(a) for a in (
        member_ids, member_profiles, interp_weights, surface_cells,
        pressure_now.reshape(rows, ny), pressure_prev.reshape(rows, ny),
        courant_sq.reshape(wx * wz, ny), stored_slabs.reshape(slots * length, points),
    )))
    placed = pltpu.HBM((rows, ny), F32)
    new, last = pl.pallas_call(
        functools.partial(last_kernel, dims),
        out_shape=(placed, placed),
        in_specs=[vmem] * 6,
        out_specs=(hbm, hbm),
        scratch_shapes=[f32(rows, ny), dma((members * wx + 1,))],
        compiler_params=pltpu.CompilerParams(vmem_limit_bytes=4 * 1024 * 1024),
    )(*kept)
    return new.reshape(pressure_now.shape), last.reshape(pressure_now.shape)


def solution(mesh):
    in_specs = (
        P("ens", "box", "slab", None), P("ens", "box", "slab", None), P("box", "slab", None), P(),
        P("ens"), P("slab", None, None), P("ens"), P(), P(),
    )
    out_specs = (P("ens", "box", "slab", None), P("ens", "box", "slab", None))
    return jax.shard_map(on_device, mesh=mesh, in_specs=in_specs, out_specs=out_specs, check_vma=False)
```
